32 devices in a mesh: rep: 1, r: 8 (over y, z), s: 4 (over x, core).
Axes of the slice: x: 2, y: 2, z: 4, core: 2. Of those that a mesh axis runs over, the one named last changes fastest.
Arguments:
- x: bfloat16 [32, 4096, 640], P(('rep', 'r', 's'))
- dy: bfloat16 [32, 4096, 640], P(('rep', 'r', 's'))
- w_gate: bfloat16 [2, 640, 2048], P(None, 's')
- w_up: bfloat16 [2, 640, 2048], P(None, 's')
- w_down: bfloat16 [2, 2048, 640], P(None, 's')
- m_w_gate: float32 [2, 640, 2048], P(None, 's')
- m_w_up: float32 [2, 640, 2048], P(None, 's')
- m_w_down: float32 [2, 2048, 640], P(None, 's')
- v_w_gate: float32 [2, 640, 2048], P(None, 's')
- v_w_up: float32 [2, 640, 2048], P(None, 's')
- v_w_down: float32 [2, 2048, 640], P(None, 's')
Outputs:
- output 1: bfloat16 [2, 640, 2048], P('rep', 's')
- output 2: bfloat16 [2, 640, 2048], P('rep', 's')
- output 3: bfloat16 [2, 2048, 640], P('rep', 's')
- output 4: float32 [2, 640, 2048], P('rep', 's')
- output 5: float32 [2, 640, 2048], P('rep', 's')
- output 6: float32 [2, 2048, 640], P('rep', 's')
- output 7: float32 [2, 640, 2048], P('rep', 's')
- output 8: float32 [2, 640, 2048], P('rep', 's')
- output 9: float32 [2, 2048, 640], P('rep', 's')
All inputs are finite; a program needn't handle non-finite values.
Results may differ from the reference program's by a relative error of at most 0.022.
Values are sent between devices in bfloat16 or wider.
A program may use at most 2 GiB of HBM per device.

```python
import jax
import jax.numpy as jnp
from jax import lax

SEQUENCES = 32
TOKENS = 4096
D = 640
FF = 2048
LAYERS = 2
NAMES = ("w_gate", "w_up", "w_down")
SHAPES = {"w_gate": (LAYERS, D, FF), "w_up": (LAYERS, D, FF), "w_down": (LAYERS, FF, D)}


def bump(key, n, height):
    away = (jnp.arange(n, dtype=jnp.int32) - jax.random.randint(key, (), 0, n, jnp.int32)) % n
    return jnp.where(away < n // 8, height, 1.0)


def together(key, own, strength):
    shared = jax.random.normal(key, own.shape[1:], jnp.float32)
    return (own + strength * shared) * lax.rsqrt(1 + strength * strength)


def setup_inputs(seed: int = 0, part: int = 0) -> dict:
    kx, kdy, ka, kb, kz, kf, kh, kl, *keys = jax.random.split(jax.random.key(seed), 8 + 3 * len(NAMES))
    kx, kdy, ka, kb = (jax.random.fold_in(k, part) for k in (kx, kdy, ka, kb))
    kw, km, kv = (keys[i::3] for i in range(3))
    shape = (SEQUENCES, TOKENS, D)
    much_x, much_dy = jax.random.uniform(kz, (2,), jnp.float32, 0.0, 1.0)
    loud = 2.0 ** jax.random.uniform(jax.random.fold_in(kz, 1), (), jnp.float32, -1.0, 2.0)
    layers = 2.0 ** jax.random.uniform(kl, (LAYERS, 1, 1), jnp.float32, -1.0, 1.0)
    x = together(ka, jax.random.normal(kx, shape, jnp.float32), much_x) * bump(kf, D, 4.0)
    dy = together(kb, jax.random.normal(kdy, shape, jnp.float32), much_dy)
    drawn = {"x": x.astype(jnp.bfloat16), "dy": (loud * dy * (SEQUENCES * TOKENS) ** -0.5).astype(jnp.bfloat16)}
    for key, name in zip(kw, NAMES, strict=True):
        w = jax.random.normal(key, SHAPES[name], jnp.float32) * SHAPES[name][1] ** -0.5
        drawn[name] = (w * {"w_gate": 1.0, "w_up": bump(kh, FF, 4.0), "w_down": layers}[name]).astype(jnp.bfloat16)
    for key, name in zip(km, NAMES, strict=True):
        drawn[f"m_{name}"] = 0.1 * jax.random.normal(key, SHAPES[name], jnp.float32)
    for key, name in zip(kv, NAMES, strict=True):
        drawn[f"v_{name}"] = jax.random.uniform(key, SHAPES[name], jnp.float32, 0.005, 0.015)
    return drawn


def matmul(a, w):
    return jnp.dot(a, w, preferred_element_type=jnp.float32).astype(jnp.bfloat16)


def normed(h):
    wide = h.astype(jnp.float32)
    scale = lax.rsqrt(jnp.mean(wide**2, -1, keepdims=True) + 1e-6)
    return (wide * scale).astype(jnp.bfloat16)


def layer(h, w):
    a = normed(h)
    gate = jnp.dot(a, w["w_gate"], preferred_element_type=jnp.float32)
    up = jnp.dot(a, w["w_up"], preferred_element_type=jnp.float32)
    return h + matmul((jax.nn.silu(gate) * up).astype(jnp.bfloat16), w["w_down"])


def adamw(w, m, v, g):
    m = 0.9 * m + 0.1 * g
    v = 0.95 * v + 0.05 * g * g
    step = m * lax.rsqrt(v + 1e-8) + 0.1 * w
    return (w - 0.02 * step).astype(jnp.bfloat16), m, v


def stack(weights, h):
    return lax.scan(lambda h, w: (layer(h, w), None), h, weights)[0]


def reference(x, dy, w_gate, w_up, w_down, m_w_gate, m_w_up, m_w_down, v_w_gate, v_w_up, v_w_down):
    weights = dict(zip(NAMES, (w_gate, w_up, w_down), strict=True))

    def take(so_far, sequence):
        h, by_y = sequence
        _, back = jax.vjp(lambda w: stack(w, h), weights)
        return jax.tree.map(lambda total, term: total + term.astype(jnp.float32), so_far, back(by_y)[0]), None

    none_yet = {name: jnp.zeros(w.shape, jnp.float32) for name, w in weights.items()}
    by_weights, _ = lax.scan(take, none_yet, (x, dy))
    gradients = [by_weights[name].astype(jnp.bfloat16).astype(jnp.float32) for name in NAMES]
    new = [
        adamw(w.astype(jnp.float32), m, v, g)
        for w, m, v, g in zip((w_gate, w_up, w_down), (m_w_gate, m_w_up, m_w_down), (v_w_gate, v_w_up, v_w_down), gradients, strict=True)
    ]
    return tuple(one[which] for which in range(3) for one in new)
```

```python
import functools

import jax
import jax.numpy as jnp
from jax import lax
from jax.experimental import pallas as pl
from jax.experimental.pallas import tpu as pltpu
from jax.sharding import PartitionSpec as P

MESH = pl.DeviceIdType.MESH
f32, bf16 = jnp.float32, jnp.bfloat16
N, D, FF, L = 4096, 640, 2048, 2
F = 512
J = FF // F
T = 1024
NT = N // T
ROWS, COLS = D // 4, F // 4
NN, TN, TT = (((1,), (0,)), ((), ())), (((0,), (0,)), ((), ())), (((1,), (1,)), ((), ()))


def dot(a, b, dims=NN):
    return lax.dot_general(a, b, dims, preferred_element_type=f32)


def of(start, size, by=8):
    return pl.ds(pl.multiple_of(start, by), size)


def normed(h):
    wide = h.astype(f32)
    return (wide * lax.rsqrt(jnp.mean(wide * wide, -1, keepdims=True) + 1e-6)).astype(bf16)


def step_kernel(
    x_h, dy_h, wg_h, wu_h, wd_h,
    ggu_h, gd_h, h1_h, a0_h, grad_h,
    a, g, act, acc, wgu, wd, stg, rc, xs, rx, ys, ry, accy, zs, rz, fin,
    gs_sem, gr_sem, w_sem, t_sem, o_sem, out_sem,
    cs, cr, xss, xrs, yss, yrs, zss, zrs, ass_, ars, bss, brs,
):
    s, r = lax.axis_index("s"), lax.axis_index("r")
    xx, core = s // 2, s % 2
    y, z = r // 4, r % 4
    sib, xn = {"s": 2 * xx + 1 - core}, {"s": 2 * (1 - xx) + core}
    yn = {"r": 4 * (1 - y) + z}
    zn = {k: {"r": 4 * y + (z + k) % 4} for k in (1, 2, 3)}

    def remote(src, dst, ss, rs, to):
        return pltpu.make_async_remote_copy(src_ref=src, dst_ref=dst, send_sem=ss, recv_sem=rs, device_id=to, device_id_type=MESH)

    barrier = pltpu.get_barrier_semaphore()
    for peer in (sib, xn, yn, zn[1], zn[2], zn[3]):
        pl.semaphore_signal(barrier, inc=1, device_id=peer, device_id_type=MESH)

    def tile(t):
        return of(t * T, T, T)

    def load_x(t):
        return pltpu.make_async_copy(x_h.at[tile(t)], g.at[tile(t)], t_sem.at[t])

    def keep_a0(t):
        return pltpu.make_async_copy(a.at[tile(t)], a0_h.at[tile(t)], o_sem.at[t])

    for t in range(NT):
        load_x(t).start()
    pl.semaphore_wait(barrier, 6)

    def part_gu(u, owner, h=None):
        cols = pl.ds(0, F) if h is None else of(256 * h, 256, 256)
        return ggu_h.at[u, :, of(owner * ROWS, ROWS, ROWS), cols]

    def part_d(u, owner, h=None):
        rows = of(owner * COLS, COLS, COLS) if h is None else of(owner * COLS + 64 * h, 64, 64)
        return gd_h.at[u, rows]

    def own_pieces(u, blocks):
        layer, j = u // J, u % J
        for which, w in enumerate((wg_h, wu_h)):
            for b in blocks:
                yield w.at[layer, :, of(b * F + j * COLS, COLS, COLS)], which, of(b * COLS, COLS, COLS)

    def own_d(u, h=None):
        layer, j = u // J, u % J
        rows = of(j * COLS, COLS, COLS) if h is None else of(j * COLS + 64 * h, 64, 64)
        return wd_h.at[layer, rows]

    def send_own(u):
        for h, path, to in ((y, 1, xn), (None, 0, sib)):
            blocks = range(4) if h is None else (2 * h, 2 * h + 1)
            for src, which, cols in own_pieces(u, blocks):
                remote(src, ggu_h.at[u, which, of(s * ROWS, ROWS, ROWS), cols], gs_sem.at[u, path, 0], gr_sem.at[u, path, 0], to).start()
            remote(own_d(u, h), part_d(u, s, h), gs_sem.at[u, path, 1], gr_sem.at[u, path, 1], to).start()

    def gather_copy(u, path, which, half=None):
        owner = {0: s, 1: s, 2: xn["s"], 3: xn["s"], 4: xn["s"]}[path]
        h = {0: None, 1: y, 2: y, 3: y, 4: 1 - y}[path]
        to = {0: sib, 1: xn, 2: yn, 3: sib, 4: sib}[path]
        ref = (part_gu, part_d)[which](u, owner, h)
        return remote(ref, ref, gs_sem.at[u, path, which], gr_sem.at[u, path, which], to)

    def forward_x(u, which):
        gather_copy(u, 1, which).wait_recv()
        gather_copy(u, 2, which).start()
        gather_copy(u, 3, which).start()

    def forward_y(u, which):
        gather_copy(u, 2, which).wait_recv()
        gather_copy(u, 4, which).start()

    def both(fn, u):
        fn(u, 0)
        fn(u, 1)

    def arrived(u, which):
        for path in (0, 3, 4):
            gather_copy(u, path, which).wait_recv()

    def load_gu(u, slot):
        for src, which, cols in own_pieces(u, range(4)):
            pltpu.make_async_copy(src, wgu.at[slot, which, of(s * ROWS, ROWS, ROWS), cols], w_sem.at[slot, 0]).start()
        for k in (1, 2, 3):
            owner = (s + k) % 4
            pltpu.make_async_copy(part_gu(u, owner), wgu.at[slot, :, of(owner * ROWS, ROWS, ROWS)], w_sem.at[slot, 0]).start()

    def load_d(u, slot):
        pltpu.make_async_copy(own_d(u), wd.at[slot, of(s * COLS, COLS, COLS)], w_sem.at[slot, 1]).start()
        for k in (1, 2, 3):
            owner = (s + k) % 4
            pltpu.make_async_copy(part_d(u, owner), wd.at[slot, of(owner * COLS, COLS, COLS)], w_sem.at[slot, 1]).start()

    def loaded(slot, which):
        ref = (wgu, wd)[which].at[slot]
        pltpu.make_async_copy(ref, ref, w_sem.at[slot, which]).wait()

    for u in range(2 * J):
        send_own(u)

    for t in range(NT):
        load_x(t).wait()
        rows = pl.ds(t * T, T)
        a[rows] = normed(g[rows])
        keep_a0(t).start()
        acc[rows] = jnp.zeros((T, D), f32)

    forward_x(0, 0)
    forward_x(0, 1)
    forward_y(0, 0)
    both(forward_x, 1)
    forward_y(0, 1)
    arrived(0, 0)
    load_gu(0, 0)
    arrived(0, 1)
    load_d(0, 0)

    def forward_chunk(c, _):
        slot = c % 2
        loaded(slot, 0)
        loaded(slot, 1)

        def body(t, _):
            rows = tile(t)
            gate, up = dot(a[rows], wgu[slot, 0]), dot(a[rows], wgu[slot, 1])
            mid = (gate / (1.0 + jnp.exp(-gate)) * up).astype(bf16)
            acc[rows] += dot(mid, wd[slot])

            @pl.when(t == 1)
            def _():
                both(forward_y, c + 1)
                both(forward_x, c + 2)

            @pl.when(t == 2)
            def _():
                for which in (0, 1):
                    arrived(c + 1, which)
                load_gu(c + 1, 1 - slot)
                load_d(c + 1, 1 - slot)

            return 0

        return lax.fori_loop(0, NT, body, 0)

    lax.fori_loop(0, J, forward_chunk, 0)

    def put_h1(t):
        return pltpu.make_async_copy(g.at[tile(t)], h1_h.at[tile(t)], out_sem.at[t])

    def load_dy(t):
        return pltpu.make_async_copy(dy_h.at[tile(t)], g.at[tile(t)], t_sem.at[t])

    for t in range(NT):
        rows = pl.ds(t * T, T)
        keep_a0(t).wait()
        h1 = (g[rows].astype(f32) + acc[rows].astype(bf16).astype(f32)).astype(bf16)
        g[rows] = h1
        put_h1(t).start()
        a[rows] = normed(h1)
        acc[rows] = jnp.zeros((T, D), f32)
        if t:
            put_h1(t - 1).wait()
            load_dy(t - 1).start()
    put_h1(NT - 1).wait()
    load_dy(NT - 1).start()

    def load_h1(t):
        return pltpu.make_async_copy(h1_h.at[tile(t)], a.at[tile(t)], out_sem.at[t])

    def load_a0(t):
        return pltpu.make_async_copy(a0_h.at[tile(t)], a.at[tile(t)], t_sem.at[t])

    def by_core(p, m):
        return remote(stg.at[p, m, 1 - core], rc.at[p, m], cs.at[p, m], cr.at[p, m], sib)

    def by_x(p, m):
        return remote(xs.at[p, m], rx.at[p, m], xss.at[p, m], xrs.at[p, m], xn)

    def by_y(p, m):
        return remote(ys.at[p, m], ry.at[p, m], yss.at[p, m], yrs.at[p, m], yn)

    def by_z(p, m, k):
        src = zs.at[p, m, of((z + k) % 4 * 80, 80, 80)]
        return remote(src, rz.at[p, m, 3 - k], zss.at[p, m, k - 1], zrs.at[p, m, 3 - k], zn[k])

    def from_z(p, m, k):
        return remote(zs.at[p, m, pl.ds(0, 80)], rz.at[p, m, k - 1], zss.at[p, m, k - 1], zrs.at[p, m, k - 1], zn[k])

    def back_z(c, p, m, k):
        ref = fin.at[c, m, of(320 * y + 80 * z, 80, 80)]
        return remote(ref, ref, ass_.at[p, m, k - 1], ars.at[p, m, 3 - k], zn[k])

    def taken_z(c, p, m, k):
        ref = fin.at[c, m, of(320 * y + 80 * ((z + k) % 4), 80, 80)]
        return remote(ref, ref, ass_.at[p, m, k - 1], ars.at[p, m, k - 1], zn[k])

    def back_y(c, p, m):
        ref = fin.at[c, m, of(320 * y, 320, 320)]
        return remote(ref, ref, bss.at[p, m], brs.at[p, m], yn)

    def s0(c, m, res):
        p = c % 2
        for o in range(4):
            if m == 0:
                stg[p, m, o % 2, o // 2] = res[:, o * COLS : (o + 1) * COLS].astype(bf16)
            else:
                for q in range(4):
                    stg[p, m, o % 2, o // 2, q * ROWS : (q + 1) * ROWS] = res[o * ROWS : (o + 1) * ROWS, q * COLS : (q + 1) * COLS].astype(bf16)
        by_core(p, m).start()

    def s1(c, m):
        p = c % 2
        by_core(p, m).wait()
        xs[p, m] = (stg[p, m, core, 1 - xx].astype(f32) + rc[p, m, 1 - xx].astype(f32)).astype(bf16)
        by_x(p, m).start()

    def s2(c, m):
        p = c % 2
        by_x(p, m).wait()

        def half(h):
            rows = of(320 * h, 320, 320)
            return stg[p, m, core, xx, rows].astype(f32) + rc[p, m, xx, rows].astype(f32) + rx[p, m, rows].astype(f32)

        ys[p, m] = half(1 - y).astype(bf16)
        by_y(p, m).start()
        accy[p, m] = half(y)

    def s3(c, m):
        p = c % 2
        by_y(p, m).wait()
        total = accy[p, m] + ry[p, m].astype(f32)
        accy[p, m] = total
        zs[p, m] = total.astype(bf16)
        for k in (1, 2, 3):
            by_z(p, m, k).start()

    def s4(c, m):
        p = c % 2
        total = accy[p, m, of(80 * z, 80, 80)]
        for k in (1, 2, 3):
            by_z(p, m, k).wait_send()
            from_z(p, m, k).wait_recv()
            total += rz[p, m, k - 1].astype(f32)
        fin[c, m, of(320 * y + 80 * z, 80, 80)] = total.astype(bf16)
        for k in (1, 2, 3):
            back_z(c, p, m, k).start()

    def s5(c, m):
        p = c % 2
        for k in (1, 2, 3):
            back_z(c, p, m, k).wait_send()
            taken_z(c, p, m, k).wait_recv()
        back_y(c, p, m).start()

    def put(c, m):
        return pltpu.make_async_copy(fin.at[c, m], grad_h.at[c, m], o_sem.at[m])

    def s6(c, m):
        p = c % 2
        back_y(c, p, m).wait_send()
        other = fin.at[c, m, of(320 * (1 - y), 320, 320)]
        remote(other, other, bss.at[p, m], brs.at[p, m], yn).wait_recv()
        put(c, m).start()

    def s7(c, m):
        put(c, m).wait()

    SLOTS = {
        "A0": ((s1, 2, 1), (s4, 2, 2), (s5, 0, 2)),
        "A1": ((s2, 0, 1), (s5, 1, 2)),
        "A2": ((s2, 1, 1), (s5, 2, 2), (s6, 0, 2)),
        "A3": ((s2, 2, 1), (s3, 0, 1), (s6, 1, 2)),
        "B0": ((s3, 1, 1), (s6, 2, 2), (s7, 0, 2)),
        "B1": ((s1, 0, 0), (s3, 2, 1), (s4, 0, 1), (s7, 1, 2)),
        "B2": ((s1, 1, 0), (s4, 1, 1), (s7, 2, 2)),
    }
    C = 2 * J

    def run(name, c):
        if isinstance(c, int):
            for fn, m, ago in SLOTS[name]:
                if 0 <= c - ago < C:
                    fn(c - ago, m)
            return
        for back in (0, 1, 2):
            todo = [(fn, m) for fn, m, ago in SLOTS[name] if ago == back]
            if todo and back == 0:
                for fn, m in todo:
                    fn(c, m)
            elif todo:

                @pl.when(c >= back)
                def _(todo=todo, back=back):
                    for fn, m in todo:
                        fn(c - back, m)

    def backward_chunk(c, _):
        slot = c % 2

        @pl.when(c == J)
        def _():
            def body(t, _):
                load_h1(t).wait()
                for i in range(2):
                    rows = of(t * T + i * (T // 2), T // 2, T // 2)
                    wide, by_a = a[rows].astype(f32), acc[rows].astype(bf16).astype(f32)
                    scale = lax.rsqrt(jnp.mean(wide * wide, -1, keepdims=True) + 1e-6)
                    along = jnp.mean(by_a * wide, -1, keepdims=True) * (scale * scale * scale)
                    by_h = (by_a * scale - wide * along).astype(bf16)
                    g[rows] = (g[rows].astype(f32) + by_h.astype(f32)).astype(bf16)
                load_a0(t).start()
                return 0

            lax.fori_loop(0, NT, body, 0)

        loaded(slot, 0)
        loaded(slot, 1)

        def body(t, _):
            rows = tile(t)

            @pl.when(c == 0)
            def _():
                load_dy(t).wait()

            @pl.when(c == J)
            def _():
                load_a0(t).wait()

            gate, up = dot(a[rows], wgu[slot, 0]), dot(a[rows], wgu[slot, 1])
            by_mid = dot(g[rows], wd[slot], TT).astype(bf16).astype(f32)
            sig = 1.0 / (1.0 + jnp.exp(-gate))
            silu = gate * sig
            act[0, rows] = (silu * up).astype(bf16)
            act[2, rows] = (by_mid * silu).astype(bf16)
            act[1, rows] = (by_mid * up * (sig + silu * (1.0 - sig))).astype(bf16)
            for k in range(NT):

                @pl.when(t == k)
                def _(k=k):
                    run(f"A{k}", c)
                    if k < 3:

                        @pl.when(c == 0)
                        def _():
                            both(forward_y, J + 1 + k)
                            if k < 2:
                                both(forward_x, J + 2 + k)
                    else:

                        @pl.when(c + 1 < J)
                        def _():
                            for which in (0, 1):
                                arrived(J + 1 + c, which)

                        @pl.when(c + 1 < C)
                        def _():
                            u = (c + 1 + J) % C
                            load_gu(u, 1 - slot)
                            load_d(u, 1 - slot)

            return 0

        lax.fori_loop(0, NT, body, 0)

        for m, lhs in enumerate((g, a, a)):
            s0(c, m, dot(lhs[...], act[m], TN))
            run(f"B{m}", c)

        @pl.when(c == J - 1)
        def _():
            for t in range(NT):
                load_h1(t).start()

        @pl.when(c < J)
        def _():
            def more(t, _):
                rows = of(t * 2048, 2048, 2048)
                acc[rows] += dot(act[1, rows], wgu[slot, 0], TT) + dot(act[2, rows], wgu[slot, 1], TT)
                return 0

            lax.fori_loop(0, N // 2048, more, 0)

        return 0

    lax.fori_loop(0, C, backward_chunk, 0)

    for c in (C, C + 1):
        for name in SLOTS:
            run(name, c)
    for u in range(2 * J):
        for path in range(5):
            for which in (0, 1):
                gather_copy(u, path, which).wait_send()


def gradients(x, dy, w_gate, w_up, w_down):
    C = L * J
    vmem, dma = pltpu.VMEM, pltpu.SemaphoreType.DMA
    hbm = pl.BlockSpec(memory_space=pl.ANY)
    out = [((C, 2, D, F), bf16), ((C, F, D), bf16), ((N, D), bf16), ((N, D), bf16), ((C, 3, D, COLS), bf16)]
    pair = [dma((2, 3)), dma((2, 3))]
    triple = [dma((2, 3, 3)), dma((2, 3, 3))]
    return pl.pallas_call(
        step_kernel,
        out_shape=[jax.ShapeDtypeStruct(*o) for o in out],
        in_specs=[hbm] * 5,
        out_specs=[hbm] * 5,
        scratch_shapes=[
            vmem((N, D), bf16), vmem((N, D), bf16), vmem((3, N, F), bf16), vmem((N, D), f32),
            vmem((2, 2, D, F), bf16), vmem((2, F, D), bf16),
            vmem((2, 3, 2, 2, D, COLS), bf16), vmem((2, 3, 2, D, COLS), bf16),
            vmem((2, 3, D, COLS), bf16), vmem((2, 3, D, COLS), bf16),
            vmem((2, 3, D // 2, COLS), bf16), vmem((2, 3, D // 2, COLS), bf16), vmem((2, 3, D // 2, COLS), f32),
            vmem((2, 3, D // 2, COLS), bf16), vmem((2, 3, 3, D // 8, COLS), bf16),
            vmem((C, 3, D, COLS), bf16),
            dma((C, 5, 2)), dma((C, 5, 2)), dma((2, 2)), dma((NT,)), dma((NT,)), dma((NT,)),
            *pair, *pair, *pair, *triple, *triple, *pair,
        ],
        compiler_params=pltpu.CompilerParams(collective_id=0, has_side_effects=True, vmem_limit_bytes=67043328),
        cost_estimate=pl.CostEstimate(flops=180 * 10**9, bytes_accessed=10**8, transcendentals=4 * 10**7),
        name="step",
    )(x, dy, w_gate, w_up, w_down)[4]


def adamw_kernel(gg, gu, gd, *refs):
    ins, outs = refs[:9], refs[9:]

    def update(which, at, g):
        w, m, v = (ins[k * 3 + which] for k in range(3))
        g = g.astype(f32)
        new_m = 0.9 * m[at] + 0.1 * g
        new_v = 0.95 * v[at] + 0.05 * g * g
        old = w[at].astype(f32)
        step = new_m * lax.rsqrt(new_v + 1e-8) + 0.1 * old
        outs[which][at] = (old - 0.02 * step).astype(bf16)
        outs[3 + which][at] = new_m
        outs[6 + which][at] = new_v

    for which, grad in enumerate((gg, gu)):
        for j in range(J):
            for q in range(4):
                update(which, (0, slice(None), slice(q * F + j * COLS, q * F + (j + 1) * COLS)), grad[0, j, 0, q])
    for j in range(gd.shape[1]):
        update(2, (0, slice(j * COLS, (j + 1) * COLS), slice(None)), gd[0, j, 0].astype(f32).T)


def adamw(grad, weights, m, v):
    parts = 2
    rows = ROWS // parts
    split = grad.reshape(L, J, 3, 4, ROWS, COLS)
    whole = grad.reshape(L, J, 3, D, COLS)
    ff = pl.BlockSpec((1, rows, FF), lambda l, i: (l, i, 0))
    down = pl.BlockSpec((1, FF // 4 // parts, D), lambda l, i: (l, i, 0))
    three = [ff, ff, down]
    shapes = [jax.ShapeDtypeStruct(o.shape, o.dtype) for o in (*weights, *m, *v)]
    return pl.pallas_call(
        adamw_kernel,
        grid=(L, parts),
        out_shape=shapes,
        in_specs=[
            pl.BlockSpec((1, J, 1, 4, rows, COLS), lambda l, i: (1 - l, 0, 1, 0, i, 0)),
            pl.BlockSpec((1, J, 1, 4, rows, COLS), lambda l, i: (1 - l, 0, 2, 0, i, 0)),
            pl.BlockSpec((1, J // parts, 1, D, COLS), lambda l, i: (1 - l, i, 0, 0, 0)),
            *three, *three, *three,
        ],
        out_specs=[*three, *three, *three],
        compiler_params=pltpu.CompilerParams(vmem_limit_bytes=60 * 2**20),
        name="adamw",
    )(split, split, whole, *weights, *m, *v)


def solution(mesh):
    def step(x, dy, *arrays):
        weights, m, v = (arrays[i : i + 3] for i in (0, 3, 6))
        grad = gradients(x[0], dy[0], *weights)
        return tuple(adamw(grad, weights, m, v))

    states, cut = P(("rep", "r", "s"), None, None), P(None, "s", None)
    return jax.shard_map(
        step,
        mesh=mesh,
        in_specs=(states, states) + (cut,) * 9,
        out_specs=(P("rep", "s", None),) * 9,
        check_vma=False,
    )
```

```python
import functools

import jax
import jax.numpy as jnp
from jax import lax
from jax.experimental import pallas as pl
from jax.experimental.pallas import tpu as pltpu
from jax.sharding import PartitionSpec as P

MESH = pl.DeviceIdType.MESH
f32, bf16 = jnp.float32, jnp.bfloat16
N, D, FF, L = 4096, 640, 2048, 2
F = 512
J = FF // F
T = 1024
NT = N // T
SUB = 256
HALVES = (pl.ds(0, SUB), pl.ds(SUB, SUB))
HALF, BLOCK = D // 2, D // 8
VLIM = 62
ROWS, COLS = D // 4, F // 4
NN, TN, TT = (((1,), (0,)), ((), ())), (((0,), (0,)), ((), ())), (((1,), (1,)), ((), ()))


def dot(a, b, dims=NN):
    return lax.dot_general(a, b, dims, preferred_element_type=f32)


def of(start, size):
    return pl.ds(pl.multiple_of(start, size), size)


def normed(h):
    wide = h.astype(f32)
    return (wide * lax.rsqrt(jnp.mean(wide * wide, -1, keepdims=True) + 1e-6)).astype(bf16)


def step_kernel(
    x_h, dy_h, wg_h, wu_h, wd_h,
    ggu_h, gd_h, h1_h, a0_h, gates_h, mids_h, grad_h,
    a, g, acc, half, wgu, wd, stg, rc, xs, rx, ys, ry, accy, zs, rz, fin,
    gs_sem, gr_sem, gs0, gr0, own0, save_sem, w_sem, t_sem, o_sem, out_sem, gate_sem, mid_sem,
    put_sem, cs, cr, xss, xrs, yss, yrs, zss, zrs, ass_, ars, bss, brs,
):
    C = 2 * J
    s, r = lax.axis_index("s"), lax.axis_index("r")
    xx, core = s // 2, s % 2
    y, z = r // 4, r % 4
    sib, xn = {"s": 2 * xx + 1 - core}, {"s": 2 * (1 - xx) + core}
    yn = {"r": 4 * (1 - y) + z}
    zn = {k: {"r": 4 * y + (z + k) % 4} for k in (1, 2, 3)}

    def remote(src, dst, ss, rs, to):
        return pltpu.make_async_remote_copy(src_ref=src, dst_ref=dst, send_sem=ss, recv_sem=rs, device_id=to, device_id_type=MESH)

    barrier = pltpu.get_barrier_semaphore()
    for peer in (sib, xn, yn, zn[1], zn[2], zn[3]):
        pl.semaphore_signal(barrier, inc=1, device_id=peer, device_id_type=MESH)

    def tile(t):
        return of(t * T, T)

    def load_x(t):
        return pltpu.make_async_copy(x_h.at[tile(t)], g.at[tile(t)], t_sem.at[t])

    def keep_a0(t):
        return pltpu.make_async_copy(a.at[tile(t)], a0_h.at[tile(t)], o_sem.at[t])

    def part_0(which, owner, h=None):
        if which < 2:
            return wgu.at[0, which, of(owner * ROWS, ROWS), pl.ds(0, F) if h is None else of(SUB * h, SUB)]
        return wd.at[0, of(owner * COLS, COLS) if h is None else of(owner * COLS + COLS // 2 * h, COLS // 2)]

    for which, w in enumerate((wg_h, wu_h)):
        for b in range(4):
            cols = pl.ds(b * COLS, COLS)
            pltpu.make_async_copy(w.at[0, :, pl.ds(b * F, COLS)], wgu.at[0, which, of(s * ROWS, ROWS), cols], own0.at[which]).start()
    pltpu.make_async_copy(wd_h.at[0, pl.ds(0, COLS)], part_0(2, s), own0.at[2]).start()

    def route(path):
        theirs = xn["s"]
        return ((s, None, sib), (s, y, xn), (theirs, y, yn), (theirs, y, sib), (theirs, 1 - y, sib))[path]

    def copy_0(path, which):
        owner, h, to = route(path)
        ref = part_0(which, owner, h)
        return remote(ref, ref, gs0.at[path, which], gr0.at[path, which], to)

    for t in range(NT):
        load_x(t).start()
    pl.semaphore_wait(barrier, 6)
    for which in range(3):
        pltpu.make_async_copy(part_0(which, s), part_0(which, s), own0.at[which]).wait()
        copy_0(1, which).start()
        copy_0(0, which).start()

    def part_gu(u, owner, h=None):
        cols = pl.ds(0, F) if h is None else of(SUB * h, SUB)
        return ggu_h.at[u, :, of(owner * ROWS, ROWS), cols]

    def part_d(u, owner, h=None):
        rows = of(owner * COLS, COLS) if h is None else of(owner * COLS + COLS // 2 * h, COLS // 2)
        return gd_h.at[u, rows]

    def own_pieces(u, blocks):
        layer, j = u // J, u % J
        for which, w in enumerate((wg_h, wu_h)):
            for b in blocks:
                yield w.at[layer, :, of(b * F + j * COLS, COLS)], which, of(b * COLS, COLS)

    def own_d(u, h=None):
        layer, j = u // J, u % J
        rows = of(j * COLS, COLS) if h is None else of(j * COLS + COLS // 2 * h, COLS // 2)
        return wd_h.at[layer, rows]

    def send_own(u):
        for h, path, to in ((y, 1, xn), (None, 0, sib)):
            blocks = range(4) if h is None else (2 * h, 2 * h + 1)
            for src, which, cols in own_pieces(u, blocks):
                remote(src, ggu_h.at[u, which, of(s * ROWS, ROWS), cols], gs_sem.at[path, 0], gr_sem.at[u, path, 0], to).start()
            remote(own_d(u, h), part_d(u, s, h), gs_sem.at[path, 1], gr_sem.at[u, path, 1], to).start()

    def gather_copy(u, path, which):
        owner, h, to = route(path)
        ref = (part_gu, part_d)[which](u, owner, h)
        return remote(ref, ref, gs_sem.at[path, which], gr_sem.at[u, path, which], to)

    def gather_sent(path, which):
        owner, h, to = route(path)
        ref = (part_gu, part_d)[which](pl.ds(1, C - 1), owner, h)
        remote(ref, ref, gs_sem.at[path, which], gr_sem.at[0, path, which], to).wait_send()

    def forward_x(u, which):
        gather_copy(u, 1, which).wait_recv()
        gather_copy(u, 2, which).start()
        gather_copy(u, 3, which).start()

    def forward_y(u, which):
        gather_copy(u, 2, which).wait_recv()
        gather_copy(u, 4, which).start()

    def both(fn, u):
        fn(u, 0)
        fn(u, 1)

    def arrived(u, which):
        for path in (0, 3, 4):
            gather_copy(u, path, which).wait_recv()

    def load_gu(u, slot):
        for src, which, cols in own_pieces(u, range(4)):
            pltpu.make_async_copy(src, wgu.at[slot, which, of(s * ROWS, ROWS), cols], w_sem.at[slot, 0]).start()
        for k in (1, 2, 3):
            owner = (s + k) % 4
            pltpu.make_async_copy(part_gu(u, owner), wgu.at[slot, :, of(owner * ROWS, ROWS)], w_sem.at[slot, 0]).start()

    def load_d(u, slot):
        pltpu.make_async_copy(own_d(u), wd.at[slot, of(s * COLS, COLS)], w_sem.at[slot, 1]).start()
        for k in (1, 2, 3):
            owner = (s + k) % 4
            pltpu.make_async_copy(part_d(u, owner), wd.at[slot, of(owner * COLS, COLS)], w_sem.at[slot, 1]).start()

    def loaded(slot, which):
        ref = (wgu, wd)[which].at[slot]
        pltpu.make_async_copy(ref, ref, w_sem.at[slot, which]).wait()

    for u in range(1, 2 * J):
        send_own(u)

    for t in range(NT):
        load_x(t).wait()
        rows = pl.ds(t * T, T)
        a[rows] = normed(g[rows])
        keep_a0(t).start()
        acc[rows] = jnp.zeros((T, D), f32)

    def forward_x0(which):
        copy_0(1, which).wait_recv()
        copy_0(2, which).start()
        copy_0(3, which).start()

    def forward_y0(which):
        copy_0(2, which).wait_recv()
        copy_0(4, which).start()

    with jax.named_scope("w0"):
        for which in range(3):
            forward_x0(which)
        for which in range(2):
            forward_y0(which)
        for which in range(2):
            for path in (0, 3, 4):
                copy_0(path, which).wait_recv()
    save_0 = (
        pltpu.make_async_copy(wgu.at[0], ggu_h.at[0], save_sem.at[0]),
        pltpu.make_async_copy(wd.at[0], gd_h.at[0], save_sem.at[1]),
    )
    save_0[0].start()

    def forward(kept, mid):
        def keep(c, t):
            return pltpu.make_async_copy(kept.at[t % 2], gates_h.at[c, :, tile(t)], gate_sem.at[t % 2])

        def keep_mid(c, t):
            return pltpu.make_async_copy(mid.at[tile(t)], mids_h.at[c, tile(t)], mid_sem.at[t])

        def chunk(c, _):
            slot = c % 2

            @pl.when(c > 0)
            def _():
                with jax.named_scope("wload"):
                    loaded(slot, 0)

            def body(t, _):
                @pl.when(c * NT + t >= 2)
                def _():
                    keep(c, t).wait()

                @pl.when(c > 0)
                def _():
                    keep_mid(c, t).wait()

                with jax.named_scope("ftile"):
                    for i in range(T // SUB):
                        rows, part = of(t * T + i * SUB, SUB), pl.ds(i * SUB, SUB)
                        for cols in HALVES:
                            gate, up = dot(a[rows], wgu[slot, 0, :, cols]), dot(a[rows], wgu[slot, 1, :, cols])
                            sig = 1.0 / (1.0 + jnp.exp(-gate))
                            silu = gate * sig
                            kept[t % 2, 0, part, cols] = silu
                            kept[t % 2, 1, part, cols] = up * (sig + silu * (1.0 - sig))
                            mid[rows, cols] = (silu * up).astype(bf16)
                keep_mid(c, t).start()
                keep(c, t).start()

                @pl.when((t == 0) & (c == 0))
                def _():
                    with jax.named_scope("f0"):
                        forward_y0(2)
                        forward_x(1, 0)

                @pl.when((t == 1) & (c == 0))
                def _():
                    with jax.named_scope("f1"):
                        forward_x(1, 1)

                @pl.when((t == 1) & (c > 0))
                def _():
                    with jax.named_scope("fa"):
                        arrived(c, 1)
                        load_d(c, slot)

                @pl.when(t == NT - 1)
                def _():
                    with jax.named_scope("f3"):
                        forward_y(c + 1, 0)

                return 0

            lax.fori_loop(0, NT, body, 0)

            def middle():
                with jax.named_scope("mid"):
                    forward_y(c + 1, 1)
                    arrived(c + 1, 0)

                    @pl.when(c == 1)
                    def _():
                        for copy in save_0:
                            copy.wait()
                        for path in range(5):
                            for which in range(3):
                                copy_0(path, which).wait_send()

                    load_gu(c + 1, 1 - slot)
                    both(forward_x, c + 2)

            @pl.when(c == 0)
            def _():
                for path in (0, 3, 4):
                    copy_0(path, 2).wait_recv()
                save_0[1].start()

            @pl.when(c > 0)
            def _():
                with jax.named_scope("wload"):
                    loaded(slot, 1)

            @pl.when(c < J - 1)
            def _():
                def down(t, _):
                    rows = of(t * 2 * T, 2 * T)
                    acc[rows] += dot(mid[rows], wd[slot])
                    pl.when(t == 0)(middle)
                    return 0

                with jax.named_scope("fdown"):
                    lax.fori_loop(0, N // (2 * T), down, 0)

            @pl.when(c == J - 1)
            def _():
                def down(t, _):
                    keep_a0(t).wait()
                    for i in range(4):
                        rows = of(t * T + i * SUB, SUB)
                        add = (acc[rows] + dot(mid[rows], wd[slot])).astype(bf16)
                        h1 = (g[rows].astype(f32) + add.astype(f32)).astype(bf16)
                        g[rows] = h1
                        a[rows] = normed(h1)
                        acc[rows] = jnp.zeros((SUB, D), f32)
                    put_h1(t).start()
                    pl.when(t == 1)(middle)

                    @pl.when(t > 0)
                    def _():
                        put_h1(t - 1).wait()
                        load_dy(t - 1).start()

                    return 0

                with jax.named_scope("fdown1"):
                    lax.fori_loop(0, NT, down, 0)
                arrived(J, 1)
                load_d(J, 0)

            return 0

        lax.fori_loop(0, J, chunk, 0)
        for t in range(NT):
            keep_mid(J - 1, t).wait()
        keep(J - 1, 0).wait()
        keep(J - 1, 1).wait()

    def put_h1(t):
        return pltpu.make_async_copy(g.at[tile(t)], h1_h.at[tile(t)], out_sem.at[t])

    def load_dy(t):
        return pltpu.make_async_copy(dy_h.at[tile(t)], g.at[tile(t)], t_sem.at[t])

    def load_h1(t):
        return pltpu.make_async_copy(h1_h.at[tile(t)], a.at[tile(t)], out_sem.at[t])

    def load_a0(t):
        return pltpu.make_async_copy(a0_h.at[tile(t)], a.at[tile(t)], t_sem.at[t])

    pl.run_scoped(forward, pltpu.VMEM((2, 2, T, F), f32), pltpu.VMEM((N, F), bf16))
    put_h1(NT - 1).wait()
    load_dy(NT - 1).start()

    def by_core(p, m):
        return remote(stg.at[p, m, 1 - core], rc.at[p, m], cs.at[p, m], cr.at[p, m], sib)

    def by_x(p, m):
        return remote(xs.at[p, m], rx.at[p, m], xss.at[p, m], xrs.at[p, m], xn)

    def by_y(p, m):
        return remote(ys.at[p, m], ry.at[p, m], yss.at[p, m], yrs.at[p, m], yn)

    def by_z(p, m, k):
        return remote(zs.at[p, m, of((z + k) % 4 * BLOCK, BLOCK)], rz.at[p, m, 3 - k], zss.at[p, m], zrs.at[p, m], zn[k])

    def by_z_all(p, m):
        return remote(zs.at[p, m, pl.ds(0, 3 * BLOCK)], rz.at[p, m], zss.at[p, m], zrs.at[p, m], zn[1])

    def back_z(c, p, m, k):
        ref = fin.at[c, m, of(HALF * y + BLOCK * z, BLOCK)]
        return remote(ref, ref, ass_.at[p, m], ars.at[p, m], zn[k])

    def back_z_all(c, p, m):
        ref = fin.at[c, m, pl.ds(0, 3 * BLOCK)]
        return remote(ref, ref, ass_.at[p, m], ars.at[p, m], zn[1])

    def back_y(c, p, m):
        ref = fin.at[c, m, of(HALF * y, HALF)]
        return remote(ref, ref, bss.at[p, m], brs.at[p, m], yn)

    def s0(c, m, res):
        p = c % 2
        for o in range(4):
            if m == 0:
                stg[p, m, o % 2, o // 2] = res[:, o * COLS : (o + 1) * COLS].astype(bf16)
            else:
                for q in range(4):
                    stg[p, m, o % 2, o // 2, q * ROWS : (q + 1) * ROWS] = res[o * ROWS : (o + 1) * ROWS, q * COLS : (q + 1) * COLS].astype(bf16)
        by_core(p, m).start()

    def s1(c, m):
        p = c % 2
        by_core(p, m).wait()
        xs[p, m] = (stg[p, m, core, 1 - xx].astype(f32) + rc[p, m, 1 - xx].astype(f32)).astype(bf16)
        by_x(p, m).start()

    def s2(c, m):
        p = c % 2
        by_x(p, m).wait()

        def sum_of(h):
            rows = of(HALF * h, HALF)
            return stg[p, m, core, xx, rows].astype(f32) + rc[p, m, xx, rows].astype(f32) + rx[p, m, rows].astype(f32)

        ys[p, m] = sum_of(1 - y).astype(bf16)
        by_y(p, m).start()
        accy[p, m] = sum_of(y)

    def s3(c, m):
        p = c % 2
        by_y(p, m).wait()
        total = accy[p, m] + ry[p, m].astype(f32)
        accy[p, m] = total
        zs[p, m] = total.astype(bf16)
        for k in zn:
            by_z(p, m, k).start()

    def s4(c, m):
        p = c % 2
        by_z_all(p, m).wait_send()
        by_z_all(p, m).wait_recv()
        total = accy[p, m, of(BLOCK * z, BLOCK)]
        for k in range(3):
            total += rz[p, m, k].astype(f32)
        fin[c, m, of(HALF * y + BLOCK * z, BLOCK)] = total.astype(bf16)
        for k in zn:
            back_z(c, p, m, k).start()

    def s5(c, m):
        p = c % 2
        back_z_all(c, p, m).wait()
        back_y(c, p, m).start()

    def put(c, m):
        return pltpu.make_async_copy(fin.at[c, m], grad_h.at[c, m], put_sem.at[0])

    def s6(c, m):
        p = c % 2
        back_y(c, p, m).wait_send()
        other = fin.at[c, m, of(HALF * (1 - y), HALF)]
        remote(other, other, bss.at[p, m], brs.at[p, m], yn).wait_recv()
        put(c, m).start()

    SLOTS = {
        "A0": "201",
        "A1": "121 412 623",
        "A2": "211",
        "A3": "",
        "H0": "502",
        "H1": "301 422",
        "H2": "100 221 512 602",
        "H3": "311",
        "H4": "110 401 522",
        "H5": "321 612",
    }
    STEPS = (None, s1, s2, s3, s4, s5, s6)
    SLOTS = {name: [tuple(map(int, word)) for word in words.split()] for name, words in SLOTS.items()}

    def run(name, c):
        with jax.named_scope("slot_" + name):
            for back in range(4):
                todo = [(STEPS[i], m) for i, m, ago in SLOTS[name] if ago == back]

                def do(todo=todo, back=back):
                    for fn, m in todo:
                        fn(c - back, m)

                if todo and back:
                    pl.when(c >= back)(do)
                elif todo:
                    do()

    def ready(i, m, c):
        start, by_x_done = ((-4.3, 1.4), (-1.4, 4.9), (1.8, 8.4))[m]
        after = start if i == 1 else by_x_done + (0.0, 4.0, 9.3, 14.6, 18.6)[i - 2]
        return after if c == C - 1 else after + 6.0 - 13.0 * (C - 1 - c)

    def finish():
        left = sorted((ready(i, m, c), i, m, c) for events in SLOTS.values() for i, m, ago in events for c in range(C - ago, C))
        sent = [(path, which) for path in range(5) for which in range(2)]
        for n, (_, i, m, c) in enumerate(left):
            with jax.named_scope(f"t{i}_{m}_{c}"):
                STEPS[i](c, m)
            if n < len(sent):
                gather_sent(*sent[n])
        pltpu.make_async_copy(fin, grad_h, put_sem.at[0]).wait()

    def gates(t):
        half = (t % 2) * 2 * T
        return acc.at[of(half, T), pl.ds(0, F)], acc.at[of(half + T, T), pl.ds(0, F)]

    def load_gates(c, t):
        return [
            pltpu.make_async_copy(gates_h.at[c - J, which, tile(t)], to, gate_sem.at[which * 2 + t % 2])
            for which, to in enumerate(gates(t))
        ]

    def backward(act):
        def chunk(c, _):
            slot = c % 2
            with jax.named_scope("wload"):
                loaded(slot, 0)
                loaded(slot, 1)

            def by_gates(rows, cols, gate, up, by_mid):
                by_mid = by_mid.astype(bf16).astype(f32)
                sig = 1.0 / (1.0 + jnp.exp(-gate))
                silu = gate * sig
                act[0, rows, cols] = (silu * up).astype(bf16)
                act[2, rows, cols] = (by_mid * silu).astype(bf16)
                act[1, rows, cols] = (by_mid * up * (sig + silu * (1.0 - sig))).astype(bf16)

            def load_mids(chunk, t):
                return pltpu.make_async_copy(mids_h.at[chunk - J, tile(t)], act.at[0, tile(t)], mid_sem.at[t])

            def product(m, h):
                lhs, rows = (g, a, a)[m], pl.ds(h * (N // 2), N // 2)
                with jax.named_scope(f"dw{m}{h}"):
                    if h == 0:
                        half[...] = dot(lhs[rows], act[m, rows], TN)
                    else:
                        s0(c, m, half[...] + dot(lhs[rows], act[m, rows], TN))
                run(f"H{2 * m + h}", c)
                if m < h:

                    @pl.when((c >= J - 1) & (c < C - 1))
                    def _():
                        for t in range(NT):
                            load_mids(c + 1, t).start()

            def body(t, _):
                @pl.when(c < J)
                def _():
                    @pl.when(c == 0)
                    def _():
                        load_dy(t).wait()

                    with jax.named_scope("btile"):
                        for i in range(4):
                            rows = of(t * T + i * SUB, SUB)
                            for cols in HALVES:
                                gate, up = dot(a[rows], wgu[slot, 0, :, cols]), dot(a[rows], wgu[slot, 1, :, cols])
                                by_gates(rows, cols, gate, up, dot(g[rows], wd[slot, cols], TT))

                @pl.when(c >= J)
                def _():
                    with jax.named_scope("gwait"):
                        for copy in load_gates(c, t):
                            copy.wait()
                    with jax.named_scope("ctile"):
                        by_up, by_gate = gates(t)
                        for i in range(T // SUB):
                            rows, part = of(t * T + i * SUB, SUB), pl.ds(i * SUB, SUB)
                            by_mid = dot(g[rows], wd[slot], TT).astype(bf16).astype(f32)
                            act[2, rows] = (by_mid * by_up[part]).astype(bf16)
                            act[1, rows] = (by_mid * by_gate[part]).astype(bf16)

                    @pl.when(t < 2)
                    def _():
                        for copy in load_gates(c, t + 2):
                            copy.start()

                    @pl.when((t >= 2) & (c + 1 < C))
                    def _():
                        for copy in load_gates(c + 1, t - 2):
                            copy.start()

                for k in range(NT):

                    @pl.when(t == k)
                    def _(k=k):
                        run(f"A{k}", c)
                        if k in (1, 2):

                            @pl.when(c >= J)
                            def _():
                                if k == 1:
                                    for t in range(NT):
                                        load_mids(c, t).wait()
                                product(0, k - 1)

                        if k < 3:

                            @pl.when(c == 0)
                            def _():
                                if k == 0:
                                    both(forward_y, J + 1)
                                    both(forward_x, J + 2)
                                if k == 2:
                                    both(forward_x, J + 3)

                            if k == 1:

                                @pl.when(c == 1)
                                def _():
                                    both(forward_y, J + 3)

                        else:

                            @pl.when(c == 0)
                            def _():
                                both(forward_y, J + 2)

                            @pl.when(c + 1 < J)
                            def _():
                                for which in (0, 1):
                                    arrived(J + 1 + c, which)

                            @pl.when(c + 1 < C)
                            def _():
                                u = (c + 1 + J) % C
                                load_gu(u, 1 - slot)
                                load_d(u, 1 - slot)

                return 0

            lax.fori_loop(0, NT, body, 0)

            @pl.when(c == J)
            def _():
                for t in range(NT):
                    load_a0(t).wait()

            for m in range(3):
                for h in range(2):
                    if m:
                        product(m, h)
                    else:
                        pl.when(c < J)(functools.partial(product, m, h))

            def by_states(rows):
                return dot(act[1, rows], wgu[slot, 0], TT) + dot(act[2, rows], wgu[slot, 1], TT)

            @pl.when(c < J - 1)
            def _():
                def more(t, _):
                    for i in range(8):
                        rows = of(t * 2 * T + i * SUB, SUB)
                        acc[rows] += by_states(rows)
                    return 0

                with jax.named_scope("p3"):
                    lax.fori_loop(0, N // (2 * T), more, 0)

            @pl.when(c == J - 1)
            def _():
                for t in range(NT):
                    load_h1(t).start()

                def more(t, _):
                    load_h1(t).wait()
                    for i in range(4):
                        rows = of(t * T + i * SUB, SUB)
                        by_a = (acc[rows] + by_states(rows)).astype(bf16).astype(f32)
                        wide = a[rows].astype(f32)
                        scale = lax.rsqrt(jnp.mean(wide * wide, -1, keepdims=True) + 1e-6)
                        along = jnp.mean(by_a * wide, -1, keepdims=True) * (scale * scale * scale)
                        by_h = (by_a * scale - wide * along).astype(bf16)
                        g[rows] = (g[rows].astype(f32) + by_h.astype(f32)).astype(bf16)
                    load_a0(t).start()

                    @pl.when(t % 2 == 1)
                    def _():
                        for copy in load_gates(J, t // 2):
                            copy.start()

                    return 0

                with jax.named_scope("normbwd"):
                    lax.fori_loop(0, NT, more, 0)

            return 0

        lax.fori_loop(0, C, chunk, 0)

    pl.run_scoped(backward, pltpu.VMEM((3, N, F), bf16))
    finish()


def gradients(x, dy, w_gate, w_up, w_down):
    C = L * J
    vmem, dma = pltpu.VMEM, pltpu.SemaphoreType.DMA
    hbm = pl.BlockSpec(memory_space=pl.ANY)
    out = [((C, 2, D, F), bf16), ((C, F, D), bf16), ((N, D), bf16), ((N, D), bf16), ((J, 2, N, F), f32), ((J, N, F), bf16), ((C, 3, D, COLS), bf16)]
    pairs = [dma((2, 3))] * 12
    return pl.pallas_call(
        step_kernel,
        out_shape=[jax.ShapeDtypeStruct(*o) for o in out],
        in_specs=[hbm] * 5,
        out_specs=[hbm] * 7,
        scratch_shapes=[
            vmem((N, D), bf16), vmem((N, D), bf16), vmem((N, D), f32), vmem((D, F), f32),
            vmem((2, 2, D, F), bf16), vmem((2, F, D), bf16),
            vmem((2, 3, 2, 2, D, COLS), bf16), vmem((2, 3, 2, D, COLS), bf16),
            vmem((2, 3, D, COLS), bf16), vmem((2, 3, D, COLS), bf16),
            vmem((2, 3, D // 2, COLS), bf16), vmem((2, 3, D // 2, COLS), bf16), vmem((2, 3, D // 2, COLS), f32),
            vmem((2, 3, D // 2, COLS), bf16), vmem((2, 3, 3, D // 8, COLS), bf16),
            vmem((C, 3, D, COLS), bf16),
            dma((5, 2)), dma((C, 5, 2)), dma((5, 3)), dma((5, 3)), dma((3,)), dma((2,)), dma((2, 2)), dma((NT,)), dma((NT,)), dma((NT,)), dma((4,)), dma((NT,)), dma((1,)),
            *pairs,
        ],
        compiler_params=pltpu.CompilerParams(collective_id=0, has_side_effects=True, vmem_limit_bytes=VLIM * 2**20),
        cost_estimate=pl.CostEstimate(flops=180 * 10**9, bytes_accessed=10**8, transcendentals=4 * 10**7),
        name="step",
    )(x, dy, w_gate, w_up, w_down)[6]


def adamw_kernel(gg, gu, gd, *refs):
    ins, outs = refs[:9], refs[9:]

    def update(which, at, g):
        w, m, v = (ins[k * 3 + which] for k in range(3))
        g = g.astype(f32)
        new_m = 0.9 * m[at] + 0.1 * g
        new_v = 0.95 * v[at] + 0.05 * g * g
        old = w[at].astype(f32)
        step = new_m * lax.rsqrt(new_v + 1e-8) + 0.1 * old
        outs[which][at] = (old - 0.02 * step).astype(bf16)
        outs[3 + which][at] = new_m
        outs[6 + which][at] = new_v

    for which, grad in enumerate((gg, gu)):
        for j in range(J):
            for q in range(4):
                update(which, (0, slice(None), slice(q * F + j * COLS, q * F + (j + 1) * COLS)), grad[0, j, 0, q])
    for j in range(gd.shape[1]):
        update(2, (0, slice(j * COLS, (j + 1) * COLS), slice(None)), gd[0, j, 0].astype(f32).T)


def adamw(grad, weights, m, v):
    parts = 2
    rows = ROWS // parts
    split = grad.reshape(L, J, 3, 4, ROWS, COLS)
    whole = grad.reshape(L, J, 3, D, COLS)
    ff = pl.BlockSpec((1, rows, FF), lambda l, i: (l, i, 0))
    down = pl.BlockSpec((1, FF // 4 // parts, D), lambda l, i: (l, i, 0))
    three = [ff, ff, down]
    shapes = [jax.ShapeDtypeStruct(o.shape, o.dtype) for o in (*weights, *m, *v)]
    return pl.pallas_call(
        adamw_kernel,
        grid=(L, parts),
        out_shape=shapes,
        in_specs=[
            pl.BlockSpec((1, J, 1, 4, rows, COLS), lambda l, i: (1 - l, 0, 1, 0, i, 0)),
            pl.BlockSpec((1, J, 1, 4, rows, COLS), lambda l, i: (1 - l, 0, 2, 0, i, 0)),
            pl.BlockSpec((1, J // parts, 1, D, COLS), lambda l, i: (1 - l, i, 0, 0, 0)),
            *three, *three, *three,
        ],
        out_specs=[*three, *three, *three],
        compiler_params=pltpu.CompilerParams(vmem_limit_bytes=56 * 2**20),
        name="adamw",
    )(split, split, whole, *weights, *m, *v)


def solution(mesh):
    def step(x, dy, *arrays):
        weights, m, v = (arrays[i : i + 3] for i in (0, 3, 6))
        grad = gradients(x[0], dy[0], *weights)
        return tuple(adamw(grad, weights, m, v))

    states, cut = P(("rep", "r", "s"), None, None), P(None, "s", None)
    return jax.shard_map(
        step,
        mesh=mesh,
        in_specs=(states, states) + (cut,) * 9,
        out_specs=(P("rep", "s", None),) * 9,
        check_vma=False,
    )
```

```python
import functools

import jax
import jax.numpy as jnp
from jax import lax
from jax.experimental import pallas as pl
from jax.experimental.pallas import tpu as pltpu
from jax.sharding import PartitionSpec as P

MESH = pl.DeviceIdType.MESH
f32, bf16 = jnp.float32, jnp.bfloat16
N, D, FF, L = 4096, 640, 2048, 2
F = 512
J = FF // F
T = 1024
NT = N // T
SUB = 256
HALVES = (pl.ds(0, SUB), pl.ds(SUB, SUB))
HALF, BLOCK = D // 2, D // 8
VLIM = 62
ROWS, COLS = D // 4, F // 4
NN, TN, TT = (((1,), (0,)), ((), ())), (((0,), (0,)), ((), ())), (((1,), (1,)), ((), ()))


def dot(a, b, dims=NN):
    return lax.dot_general(a, b, dims, preferred_element_type=f32)


def of(start, size):
    return pl.ds(pl.multiple_of(start, size), size)


def normed(h):
    wide = h.astype(f32)
    return (wide * lax.rsqrt(jnp.mean(wide * wide, -1, keepdims=True) + 1e-6)).astype(bf16)


def step_kernel(
    x_h, dy_h, wg_h, wu_h, wd_h,
    ggu_h, gd_h, h1_h, a0_h, gates_h, mids_h, grad_h,
    a, g, acc, half, wgu, wd, stg, rc, xs, rx, ys, ry, accy, zs, rz, fin,
    gs_sem, gr_sem, gs0, gr0, own0, save_sem, w_sem, t_sem, o_sem, out_sem, gate_sem, mid_sem,
    put_sem, cs, cr, xss, xrs, yss, yrs, zss, zrs, ass_, ars, bss, brs,
):
    C = 2 * J
    s, r = lax.axis_index("s"), lax.axis_index("r")
    xx, core = s // 2, s % 2
    y, z = r // 4, r % 4
    sib, xn = {"s": 2 * xx + 1 - core}, {"s": 2 * (1 - xx) + core}
    yn = {"r": 4 * (1 - y) + z}
    zn = {k: {"r": 4 * y + (z + k) % 4} for k in (1, 2, 3)}

    def remote(src, dst, ss, rs, to):
        return pltpu.make_async_remote_copy(src_ref=src, dst_ref=dst, send_sem=ss, recv_sem=rs, device_id=to, device_id_type=MESH)

    barrier = pltpu.get_barrier_semaphore()
    for peer in (sib, xn, yn, zn[1], zn[2], zn[3]):
        pl.semaphore_signal(barrier, inc=1, device_id=peer, device_id_type=MESH)

    def tile(t):
        return of(t * T, T)

    def load_x(t):
        return pltpu.make_async_copy(x_h.at[tile(t)], g.at[tile(t)], t_sem.at[t])

    def keep_a0(t):
        return pltpu.make_async_copy(a.at[tile(t)], a0_h.at[tile(t)], o_sem.at[t])

    def part_0(which, owner, h=None):
        if which < 2:
            return wgu.at[0, which, of(owner * ROWS, ROWS), pl.ds(0, F) if h is None else of(SUB * h, SUB)]
        return wd.at[0, of(owner * COLS, COLS) if h is None else of(owner * COLS + COLS // 2 * h, COLS // 2)]

    for which, w in enumerate((wg_h, wu_h)):
        for b in range(4):
            cols = pl.ds(b * COLS, COLS)
            pltpu.make_async_copy(w.at[0, :, pl.ds(b * F, COLS)], wgu.at[0, which, of(s * ROWS, ROWS), cols], own0.at[which]).start()
    pltpu.make_async_copy(wd_h.at[0, pl.ds(0, COLS)], part_0(2, s), own0.at[2]).start()

    def route(path):
        theirs = xn["s"]
        return ((s, None, sib), (s, y, xn), (theirs, y, yn), (theirs, y, sib), (theirs, 1 - y, sib))[path]

    def copy_0(path, which):
        owner, h, to = route(path)
        ref = part_0(which, owner, h)
        return remote(ref, ref, gs0.at[path, which], gr0.at[path, which], to)

    for t in range(NT):
        load_x(t).start()
    pl.semaphore_wait(barrier, 6)
    for which in range(3):
        pltpu.make_async_copy(part_0(which, s), part_0(which, s), own0.at[which]).wait()
        copy_0(1, which).start()
        copy_0(0, which).start()

    def part_gu(u, owner, h=None):
        cols = pl.ds(0, F) if h is None else of(SUB * h, SUB)
        return ggu_h.at[u, :, of(owner * ROWS, ROWS), cols]

    def part_d(u, owner, h=None):
        rows = of(owner * COLS, COLS) if h is None else of(owner * COLS + COLS // 2 * h, COLS // 2)
        return gd_h.at[u, rows]

    def own_pieces(u, blocks):
        layer, j = u // J, u % J
        for which, w in enumerate((wg_h, wu_h)):
            for b in blocks:
                yield w.at[layer, :, of(b * F + j * COLS, COLS)], which, of(b * COLS, COLS)

    def own_d(u, h=None):
        layer, j = u // J, u % J
        rows = of(j * COLS, COLS) if h is None else of(j * COLS + COLS // 2 * h, COLS // 2)
        return wd_h.at[layer, rows]

    def send_own(u):
        for h, path, to in ((y, 1, xn), (None, 0, sib)):
            blocks = range(4) if h is None else (2 * h, 2 * h + 1)
            for src, which, cols in own_pieces(u, blocks):
                remote(src, ggu_h.at[u, which, of(s * ROWS, ROWS), cols], gs_sem.at[path, 0], gr_sem.at[u, path, 0], to).start()
            remote(own_d(u, h), part_d(u, s, h), gs_sem.at[path, 1], gr_sem.at[u, path, 1], to).start()

    def gather_copy(u, path, which):
        owner, h, to = route(path)
        ref = (part_gu, part_d)[which](u, owner, h)
        return remote(ref, ref, gs_sem.at[path, which], gr_sem.at[u, path, which], to)

    def gather_sent(path, which):
        owner, h, to = route(path)
        ref = (part_gu, part_d)[which](pl.ds(1, C - 1), owner, h)
        remote(ref, ref, gs_sem.at[path, which], gr_sem.at[0, path, which], to).wait_send()

    def forward_x(u, which):
        gather_copy(u, 1, which).wait_recv()
        gather_copy(u, 2, which).start()
        gather_copy(u, 3, which).start()

    def forward_y(u, which):
        gather_copy(u, 2, which).wait_recv()
        gather_copy(u, 4, which).start()

    def both(fn, u):
        fn(u, 0)
        fn(u, 1)

    def arrived(u, which):
        for path in (0, 3, 4):
            gather_copy(u, path, which).wait_recv()

    def load_gu(u, slot):
        for src, which, cols in own_pieces(u, range(4)):
            pltpu.make_async_copy(src, wgu.at[slot, which, of(s * ROWS, ROWS), cols], w_sem.at[slot, 0]).start()
        for k in (1, 2, 3):
            owner = (s + k) % 4
            pltpu.make_async_copy(part_gu(u, owner), wgu.at[slot, :, of(owner * ROWS, ROWS)], w_sem.at[slot, 0]).start()

    def load_d(u, slot):
        pltpu.make_async_copy(own_d(u), wd.at[slot, of(s * COLS, COLS)], w_sem.at[slot, 1]).start()
        for k in (1, 2, 3):
            owner = (s + k) % 4
            pltpu.make_async_copy(part_d(u, owner), wd.at[slot, of(owner * COLS, COLS)], w_sem.at[slot, 1]).start()

    def loaded(slot, which):
        ref = (wgu, wd)[which].at[slot]
        pltpu.make_async_copy(ref, ref, w_sem.at[slot, which]).wait()

    for u in range(1, 2 * J):
        send_own(u)

    for t in range(NT):
        load_x(t).wait()
        rows = pl.ds(t * T, T)
        a[rows] = normed(g[rows])
        keep_a0(t).start()
        acc[rows] = jnp.zeros((T, D), f32)

    def forward_x0(which):
        copy_0(1, which).wait_recv()
        copy_0(2, which).start()
        copy_0(3, which).start()

    def forward_y0(which):
        copy_0(2, which).wait_recv()
        copy_0(4, which).start()

    with jax.named_scope("w0"):
        for which in range(3):
            forward_x0(which)
        for which in range(2):
            forward_y0(which)
        for which in range(2):
            for path in (0, 3, 4):
                copy_0(path, which).wait_recv()
    save_0 = (
        pltpu.make_async_copy(wgu.at[0], ggu_h.at[0], save_sem.at[0]),
        pltpu.make_async_copy(wd.at[0], gd_h.at[0], save_sem.at[1]),
    )
    save_0[0].start()

    def forward(kept, mid):
        def keep(c, t):
            return pltpu.make_async_copy(kept.at[t % 2], gates_h.at[c, :, tile(t)], gate_sem.at[t % 2])

        def keep_half(c, t, h):
            rows, size = h * (T // 2), T // 2
            to = gates_h.at[c, :, of(t * T + rows, size)]
            return pltpu.make_async_copy(kept.at[t % 2, :, pl.ds(rows, size)], to, gate_sem.at[t % 2])

        def keep_mid(c, t):
            return pltpu.make_async_copy(mid.at[tile(t)], mids_h.at[c, tile(t)], mid_sem.at[t])

        def chunk(c, _):
            slot = c % 2

            @pl.when(c > 0)
            def _():
                with jax.named_scope("wload"):
                    loaded(slot, 0)

            def body(t, _):
                @pl.when(c * NT + t >= 2)
                def _():
                    keep(c, t).wait()

                @pl.when(c > 0)
                def _():
                    keep_mid(c, t).wait()

                with jax.named_scope("ftile"):
                    for i in range(T // SUB):
                        rows, part = of(t * T + i * SUB, SUB), pl.ds(i * SUB, SUB)
                        for cols in HALVES:
                            gate, up = dot(a[rows], wgu[slot, 0, :, cols]), dot(a[rows], wgu[slot, 1, :, cols])
                            sig = 1.0 / (1.0 + jnp.exp(-gate))
                            silu = gate * sig
                            kept[t % 2, 0, part, cols] = silu
                            kept[t % 2, 1, part, cols] = up * (sig + silu * (1.0 - sig))
                            mid[rows, cols] = (silu * up).astype(bf16)
                        if i % 2:
                            keep_half(c, t, i // 2).start()
                keep_mid(c, t).start()

                @pl.when((t == 0) & (c == 0))
                def _():
                    with jax.named_scope("f0"):
                        forward_y0(2)
                        forward_x(1, 0)

                @pl.when((t == 1) & (c == 0))
                def _():
                    with jax.named_scope("f1"):
                        forward_x(1, 1)

                @pl.when((t == 1) & (c > 0))
                def _():
                    with jax.named_scope("fa"):
                        arrived(c, 1)
                        load_d(c, slot)

                @pl.when(t == NT - 1)
                def _():
                    with jax.named_scope("f3"):
                        forward_y(c + 1, 0)

                return 0

            lax.fori_loop(0, NT, body, 0)

            def middle():
                with jax.named_scope("mid"):
                    forward_y(c + 1, 1)
                    arrived(c + 1, 0)

                    @pl.when(c == 1)
                    def _():
                        for copy in save_0:
                            copy.wait()
                        for path in range(5):
                            for which in range(3):
                                copy_0(path, which).wait_send()

                    load_gu(c + 1, 1 - slot)
                    both(forward_x, c + 2)

            @pl.when(c == 0)
            def _():
                for path in (0, 3, 4):
                    copy_0(path, 2).wait_recv()
                save_0[1].start()

            @pl.when(c > 0)
            def _():
                with jax.named_scope("wload"):
                    loaded(slot, 1)

            @pl.when(c < J - 1)
            def _():
                def down(t, _):
                    rows = of(t * 2 * T, 2 * T)
                    acc[rows] += dot(mid[rows], wd[slot])
                    pl.when(t == 0)(middle)
                    return 0

                with jax.named_scope("fdown"):
                    lax.fori_loop(0, N // (2 * T), down, 0)

            @pl.when(c == J - 1)
            def _():
                def down(t, _):
                    keep_a0(t).wait()
                    for i in range(4):
                        rows = of(t * T + i * SUB, SUB)
                        add = (acc[rows] + dot(mid[rows], wd[slot])).astype(bf16)
                        h1 = (g[rows].astype(f32) + add.astype(f32)).astype(bf16)
                        g[rows] = h1
                        a[rows] = normed(h1)
                        acc[rows] = jnp.zeros((SUB, D), f32)
                    put_h1(t).start()
                    pl.when(t == 1)(middle)

                    @pl.when(t == NT - 1)
                    def _():
                        arrived(J, 1)
                        load_d(J, 0)


                    @pl.when(t > 0)
                    def _():
                        put_h1(t - 1).wait()
                        load_dy(t - 1).start()

                    return 0

                with jax.named_scope("fdown1"):
                    lax.fori_loop(0, NT, down, 0)

            return 0

        lax.fori_loop(0, J, chunk, 0)
        for t in range(NT):
            keep_mid(J - 1, t).wait()
        keep(J - 1, 0).wait()
        keep(J - 1, 1).wait()

    def put_h1(t):
        return pltpu.make_async_copy(g.at[tile(t)], h1_h.at[tile(t)], out_sem.at[t])

    def load_dy(t):
        return pltpu.make_async_copy(dy_h.at[tile(t)], g.at[tile(t)], t_sem.at[t])

    def load_h1(t):
        return pltpu.make_async_copy(h1_h.at[tile(t)], a.at[tile(t)], out_sem.at[t])

    def load_a0(t):
        return pltpu.make_async_copy(a0_h.at[tile(t)], a.at[tile(t)], t_sem.at[t])

    pl.run_scoped(forward, pltpu.VMEM((2, 2, T, F), f32), pltpu.VMEM((N, F), bf16))
    put_h1(NT - 1).wait()
    load_dy(NT - 1).start()

    def by_core(p, m):
        return remote(stg.at[p, m, 1 - core], rc.at[p, m], cs.at[p, m], cr.at[p, m], sib)

    def by_x(p, m):
        return remote(xs.at[p, m], rx.at[p, m], xss.at[p, m], xrs.at[p, m], xn)

    def by_y(p, m):
        return remote(ys.at[p, m], ry.at[p, m], yss.at[p, m], yrs.at[p, m], yn)

    def by_z(p, m, k):
        return remote(zs.at[p, m, of((z + k) % 4 * BLOCK, BLOCK)], rz.at[p, m, 3 - k], zss.at[p, m], zrs.at[p, m], zn[k])

    def by_z_all(p, m):
        return remote(zs.at[p, m, pl.ds(0, 3 * BLOCK)], rz.at[p, m], zss.at[p, m], zrs.at[p, m], zn[1])

    def back_z(c, p, m, k):
        ref = fin.at[c, m, of(HALF * y + BLOCK * z, BLOCK)]
        return remote(ref, ref, ass_.at[p, m], ars.at[p, m], zn[k])

    def back_z_all(c, p, m):
        ref = fin.at[c, m, pl.ds(0, 3 * BLOCK)]
        return remote(ref, ref, ass_.at[p, m], ars.at[p, m], zn[1])

    def back_y(c, p, m):
        ref = fin.at[c, m, of(HALF * y, HALF)]
        return remote(ref, ref, bss.at[p, m], brs.at[p, m], yn)

    def s0(c, m, res):
        p = c % 2
        for o in range(4):
            if m == 0:
                stg[p, m, o % 2, o // 2] = res[:, o * COLS : (o + 1) * COLS].astype(bf16)
            else:
                for q in range(4):
                    stg[p, m, o % 2, o // 2, q * ROWS : (q + 1) * ROWS] = res[o * ROWS : (o + 1) * ROWS, q * COLS : (q + 1) * COLS].astype(bf16)
        by_core(p, m).start()

    def s1(c, m):
        p = c % 2
        by_core(p, m).wait()
        xs[p, m] = (stg[p, m, core, 1 - xx].astype(f32) + rc[p, m, 1 - xx].astype(f32)).astype(bf16)
        by_x(p, m).start()

    def s2(c, m):
        p = c % 2
        by_x(p, m).wait()

        def sum_of(h):
            rows = of(HALF * h, HALF)
            return stg[p, m, core, xx, rows].astype(f32) + rc[p, m, xx, rows].astype(f32) + rx[p, m, rows].astype(f32)

        ys[p, m] = sum_of(1 - y).astype(bf16)
        by_y(p, m).start()
        accy[p, m] = sum_of(y)

    def s3(c, m):
        p = c % 2
        by_y(p, m).wait()
        total = accy[p, m] + ry[p, m].astype(f32)
        accy[p, m] = total
        zs[p, m] = total.astype(bf16)
        for k in zn:
            by_z(p, m, k).start()

    def s4(c, m):
        p = c % 2
        by_z_all(p, m).wait_send()
        by_z_all(p, m).wait_recv()
        total = accy[p, m, of(BLOCK * z, BLOCK)]
        for k in range(3):
            total += rz[p, m, k].astype(f32)
        fin[c, m, of(HALF * y + BLOCK * z, BLOCK)] = total.astype(bf16)
        for k in zn:
            back_z(c, p, m, k).start()

    def s5(c, m):
        p = c % 2
        back_z_all(c, p, m).wait()
        back_y(c, p, m).start()

    def put(c, m):
        return pltpu.make_async_copy(fin.at[c, m], grad_h.at[c, m], put_sem.at[0])

    def s6(c, m):
        p = c % 2
        back_y(c, p, m).wait_send()
        other = fin.at[c, m, of(HALF * (1 - y), HALF)]
        remote(other, other, bss.at[p, m], brs.at[p, m], yn).wait_recv()
        put(c, m).start()

    SLOTS = {
        "A0": "201",
        "A1": "121 412 623",
        "A2": "211",
        "A3": "",
        "H0": "502",
        "H1": "301 422",
        "H2": "100 221 512 602",
        "H3": "311",
        "H4": "110 401 522",
        "H5": "321 612",
    }
    STEPS = (None, s1, s2, s3, s4, s5, s6)
    SLOTS = {name: [tuple(map(int, word)) for word in words.split()] for name, words in SLOTS.items()}

    def run(name, c):
        with jax.named_scope("slot_" + name):
            for back in range(4):
                todo = [(STEPS[i], m) for i, m, ago in SLOTS[name] if ago == back]

                def do(todo=todo, back=back):
                    for fn, m in todo:
                        fn(c - back, m)

                if todo and back:
                    pl.when(c >= back)(do)
                elif todo:
                    do()

    def ready(i, m, c):
        start = 3 * m - 4.3
        by_x_done = start + 5.7 + 0.5 * m
        after = start if i == 1 else by_x_done + (0.0, 4.0, 9.3, 14.6, 18.6)[i - 2]
        return after if c == C - 1 else after + 6.0 - 13.0 * (C - 1 - c)

    def finish():
        left = sorted((ready(i, m, c), i, m, c) for events in SLOTS.values() for i, m, ago in events for c in range(C - ago, C))
        sent = [(path, which) for path in range(5) for which in range(2)]
        for n, (_, i, m, c) in enumerate(left):
            with jax.named_scope(f"t{i}_{m}_{c}"):
                STEPS[i](c, m)
            if n < len(sent):
                gather_sent(*sent[n])
        pltpu.make_async_copy(fin, grad_h, put_sem.at[0]).wait()

    def gates(t):
        half = (t % 2) * 2 * T
        return acc.at[of(half, T), pl.ds(0, F)], acc.at[of(half + T, T), pl.ds(0, F)]

    def load_gates(c, t):
        return [
            pltpu.make_async_copy(gates_h.at[c - J, which, tile(t)], to, gate_sem.at[which * 2 + t % 2])
            for which, to in enumerate(gates(t))
        ]

    def backward(act):
        def chunk(c, _):
            slot = c % 2
            with jax.named_scope("wload"):
                loaded(slot, 0)
                loaded(slot, 1)

            def by_gates(rows, cols, gate, up, by_mid):
                by_mid = by_mid.astype(bf16).astype(f32)
                sig = 1.0 / (1.0 + jnp.exp(-gate))
                silu = gate * sig
                act[0, rows, cols] = (silu * up).astype(bf16)
                act[2, rows, cols] = (by_mid * silu).astype(bf16)
                act[1, rows, cols] = (by_mid * up * (sig + silu * (1.0 - sig))).astype(bf16)

            def load_mids(chunk, t):
                return pltpu.make_async_copy(mids_h.at[chunk - J, tile(t)], act.at[0, tile(t)], mid_sem.at[t])

            def product(m, h):
                lhs, rows = (g, a, a)[m], pl.ds(h * (N // 2), N // 2)
                with jax.named_scope(f"dw{m}{h}"):
                    if h == 0:
                        half[...] = dot(lhs[rows], act[m, rows], TN)
                    else:
                        s0(c, m, half[...] + dot(lhs[rows], act[m, rows], TN))
                run(f"H{2 * m + h}", c)
                if m < h:

                    @pl.when((c >= J - 1) & (c < C - 1))
                    def _():
                        for t in range(NT):
                            load_mids(c + 1, t).start()

            def body(t, _):
                @pl.when(c < J)
                def _():
                    @pl.when(c == 0)
                    def _():
                        load_dy(t).wait()

                    with jax.named_scope("btile"):
                        for i in range(4):
                            rows = of(t * T + i * SUB, SUB)
                            for cols in HALVES:
                                gate, up = dot(a[rows], wgu[slot, 0, :, cols]), dot(a[rows], wgu[slot, 1, :, cols])
                                by_gates(rows, cols, gate, up, dot(g[rows], wd[slot, cols], TT))

                @pl.when(c >= J)
                def _():
                    with jax.named_scope("gwait"):
                        for copy in load_gates(c, t):
                            copy.wait()
                    with jax.named_scope("ctile"):
                        by_up, by_gate = gates(t)
                        for i in range(T // SUB):
                            rows, part = of(t * T + i * SUB, SUB), pl.ds(i * SUB, SUB)
                            by_mid = dot(g[rows], wd[slot], TT).astype(bf16).astype(f32)
                            act[2, rows] = (by_mid * by_up[part]).astype(bf16)
                            act[1, rows] = (by_mid * by_gate[part]).astype(bf16)

                    @pl.when(t < 2)
                    def _():
                        for copy in load_gates(c, t + 2):
                            copy.start()

                    @pl.when((t >= 2) & (c + 1 < C))
                    def _():
                        for copy in load_gates(c + 1, t - 2):
                            copy.start()

                for k in range(NT):

                    @pl.when(t == k)
                    def _(k=k):
                        run(f"A{k}", c)
                        if k in (1, 2):

                            @pl.when(c >= J)
                            def _():
                                if k == 1:
                                    for t in range(NT):
                                        load_mids(c, t).wait()
                                product(0, k - 1)

                        if k < 3:

                            @pl.when(c == 0)
                            def _():
                                if k == 0:
                                    both(forward_y, J + 1)
                                    both(forward_x, J + 2)
                                if k == 2:
                                    both(forward_x, J + 3)

                            if k == 1:

                                @pl.when(c == 1)
                                def _():
                                    both(forward_y, J + 3)

                        else:

                            @pl.when(c == 0)
                            def _():
                                both(forward_y, J + 2)

                            @pl.when(c + 1 < J)
                            def _():
                                for which in (0, 1):
                                    arrived(J + 1 + c, which)

                            @pl.when(c + 1 < C)
                            def _():
                                u = (c + 1 + J) % C
                                load_gu(u, 1 - slot)
                                load_d(u, 1 - slot)

                return 0

            lax.fori_loop(0, NT, body, 0)

            @pl.when(c == J)
            def _():
                for t in range(NT):
                    load_a0(t).wait()

            for m in range(3):
                for h in range(2):
                    if m:
                        product(m, h)
                    else:
                        pl.when(c < J)(functools.partial(product, m, h))

            def by_states(rows):
                return dot(act[1, rows], wgu[slot, 0], TT) + dot(act[2, rows], wgu[slot, 1], TT)

            @pl.when(c < J - 1)
            def _():
                def more(t, _):
                    for i in range(8):
                        rows = of(t * 2 * T + i * SUB, SUB)
                        acc[rows] += by_states(rows)
                    return 0

                with jax.named_scope("p3"):
                    lax.fori_loop(0, N // (2 * T), more, 0)

            @pl.when(c == J - 1)
            def _():
                for t in range(NT):
                    load_h1(t).start()

                def more(t, _):
                    load_h1(t).wait()
                    for i in range(4):
                        rows = of(t * T + i * SUB, SUB)
                        by_a = (acc[rows] + by_states(rows)).astype(bf16).astype(f32)
                        wide = a[rows].astype(f32)
                        scale = lax.rsqrt(jnp.mean(wide * wide, -1, keepdims=True) + 1e-6)
                        along = jnp.mean(by_a * wide, -1, keepdims=True) * (scale * scale * scale)
                        by_h = (by_a * scale - wide * along).astype(bf16)
                        g[rows] = (g[rows].astype(f32) + by_h.astype(f32)).astype(bf16)
                    load_a0(t).start()

                    @pl.when(t % 2 == 1)
                    def _():
                        for copy in load_gates(J, t // 2):
                            copy.start()

                    return 0

                with jax.named_scope("normbwd"):
                    lax.fori_loop(0, NT, more, 0)

            return 0

        lax.fori_loop(0, C, chunk, 0)

    pl.run_scoped(backward, pltpu.VMEM((3, N, F), bf16))
    finish()


def gradients(x, dy, w_gate, w_up, w_down):
    C = L * J
    vmem, dma = pltpu.VMEM, pltpu.SemaphoreType.DMA
    hbm = pl.BlockSpec(memory_space=pl.ANY)
    out = [((C, 2, D, F), bf16), ((C, F, D), bf16), ((N, D), bf16), ((N, D), bf16), ((J, 2, N, F), f32), ((J, N, F), bf16), ((C, 3, D, COLS), bf16)]
    pairs = [dma((2, 3))] * 12
    return pl.pallas_call(
        step_kernel,
        out_shape=[jax.ShapeDtypeStruct(*o) for o in out],
        in_specs=[hbm] * 5,
        out_specs=[hbm] * 7,
        scratch_shapes=[
            vmem((N, D), bf16), vmem((N, D), bf16), vmem((N, D), f32), vmem((D, F), f32),
            vmem((2, 2, D, F), bf16), vmem((2, F, D), bf16),
            vmem((2, 3, 2, 2, D, COLS), bf16), vmem((2, 3, 2, D, COLS), bf16),
            vmem((2, 3, D, COLS), bf16), vmem((2, 3, D, COLS), bf16),
            vmem((2, 3, D // 2, COLS), bf16), vmem((2, 3, D // 2, COLS), bf16), vmem((2, 3, D // 2, COLS), f32),
            vmem((2, 3, D // 2, COLS), bf16), vmem((2, 3, 3, D // 8, COLS), bf16),
            vmem((C, 3, D, COLS), bf16),
            dma((5, 2)), dma((C, 5, 2)), dma((5, 3)), dma((5, 3)), dma((3,)), dma((2,)), dma((2, 2)), dma((NT,)), dma((NT,)), dma((NT,)), dma((4,)), dma((NT,)), dma((1,)),
            *pairs,
        ],
        compiler_params=pltpu.CompilerParams(collective_id=0, has_side_effects=True, vmem_limit_bytes=VLIM * 2**20),
        cost_estimate=pl.CostEstimate(flops=180 * 10**9, bytes_accessed=10**8, transcendentals=4 * 10**7),
        name="step",
    )(x, dy, w_gate, w_up, w_down)[6]


def adamw_kernel(gg, gu, gd, *refs):
    ins, outs = refs[:9], refs[9:]

    def update(which, at, g):
        w, m, v = (ins[k * 3 + which] for k in range(3))
        g = g.astype(f32)
        new_m = 0.9 * m[at] + 0.1 * g
        new_v = 0.95 * v[at] + 0.05 * g * g
        old = w[at].astype(f32)
        step = new_m * lax.rsqrt(new_v + 1e-8) + 0.1 * old
        outs[which][at] = (old - 0.02 * step).astype(bf16)
        outs[3 + which][at] = new_m
        outs[6 + which][at] = new_v

    for which, grad in enumerate((gg, gu)):
        for j in range(J):
            for q in range(4):
                update(which, (0, slice(None), slice(q * F + j * COLS, q * F + (j + 1) * COLS)), grad[0, j, 0, q])
    for j in range(gd.shape[1]):
        update(2, (0, slice(j * COLS, (j + 1) * COLS), slice(None)), gd[0, j, 0].astype(f32).T)


def adamw(grad, weights, m, v):
    parts = 2
    rows = ROWS // parts
    split = grad.reshape(L, J, 3, 4, ROWS, COLS)
    whole = grad.reshape(L, J, 3, D, COLS)
    ff = pl.BlockSpec((1, rows, FF), lambda l, i: (l, i, 0))
    down = pl.BlockSpec((1, FF // 4 // parts, D), lambda l, i: (l, i, 0))
    three = [ff, ff, down]
    shapes = [jax.ShapeDtypeStruct(o.shape, o.dtype) for o in (*weights, *m, *v)]
    return pl.pallas_call(
        adamw_kernel,
        grid=(L, parts),
        out_shape=shapes,
        in_specs=[
            pl.BlockSpec((1, J, 1, 4, rows, COLS), lambda l, i: (1 - l, 0, 1, 0, i, 0)),
            pl.BlockSpec((1, J, 1, 4, rows, COLS), lambda l, i: (1 - l, 0, 2, 0, i, 0)),
            pl.BlockSpec((1, J // parts, 1, D, COLS), lambda l, i: (1 - l, i, 0, 0, 0)),
            *three, *three, *three,
        ],
        out_specs=[*three, *three, *three],
        compiler_params=pltpu.CompilerParams(vmem_limit_bytes=56 * 2**20),
        name="adamw",
    )(split, split, whole, *weights, *m, *v)


def solution(mesh):
    def step(x, dy, *arrays):
        weights, m, v = (arrays[i : i + 3] for i in (0, 3, 6))
        grad = gradients(x[0], dy[0], *weights)
        return tuple(adamw(grad, weights, m, v))

    states, cut = P(("rep", "r", "s"), None, None), P(None, "s", None)
    return jax.shard_map(
        step,
        mesh=mesh,
        in_specs=(states, states) + (cut,) * 9,
        out_specs=(P("rep", "s", None),) * 9,
        check_vma=False,
    )
```

```python
import functools

import jax
import jax.numpy as jnp
from jax import lax
from jax.experimental import pallas as pl
from jax.experimental.pallas import tpu as pltpu
from jax.sharding import PartitionSpec as P

MESH = pl.DeviceIdType.MESH
f32, bf16 = jnp.float32, jnp.bfloat16
N, D, FF, L = 4096, 640, 2048, 2
F = 512
J = FF // F
T = 1024
NT = N // T
SUB = 256
HALVES = (pl.ds(0, SUB), pl.ds(SUB, SUB))
HALF, BLOCK = D // 2, D // 8
VLIM = 62
ROWS, COLS = D // 4, F // 4
NN, TN, TT = (((1,), (0,)), ((), ())), (((0,), (0,)), ((), ())), (((1,), (1,)), ((), ()))


def dot(a, b, dims=NN):
    return lax.dot_general(a, b, dims, preferred_element_type=f32)


def of(start, size):
    return pl.ds(pl.multiple_of(start, size), size)


def normed(h):
    wide = h.astype(f32)
    return (wide * lax.rsqrt(jnp.mean(wide * wide, -1, keepdims=True) + 1e-6)).astype(bf16)


def step_kernel(
    x_h, dy_h, wg_h, wu_h, wd_h,
    ggu_h, gd_h, h1_h, a0_h, gates_h, mids_h, grad_h,
    a, g, acc, half, wgu, wd, stg, rc, xs, rx, ys, ry, accy, zs, rz, fin,
    gs_sem, gr_sem, gs0, gr0, own0, save_sem, w_sem, t_sem, o_sem, out_sem, gate_sem, mid_sem,
    put_sem, cs, cr, xss, xrs, yss, yrs, zss, zrs, ass_, ars, bss, brs,
):
    C = 2 * J
    s, r = lax.axis_index("s"), lax.axis_index("r")
    xx, core = s // 2, s % 2
    y, z = r // 4, r % 4
    sib, xn = {"s": 2 * xx + 1 - core}, {"s": 2 * (1 - xx) + core}
    yn = {"r": 4 * (1 - y) + z}
    zn = {k: {"r": 4 * y + (z + k) % 4} for k in (1, 2, 3)}

    def remote(src, dst, ss, rs, to):
        return pltpu.make_async_remote_copy(src_ref=src, dst_ref=dst, send_sem=ss, recv_sem=rs, device_id=to, device_id_type=MESH)

    barrier = pltpu.get_barrier_semaphore()
    for peer in (sib, xn, yn, zn[1], zn[2], zn[3]):
        pl.semaphore_signal(barrier, inc=1, device_id=peer, device_id_type=MESH)

    def tile(t):
        return of(t * T, T)

    def load_x(t):
        return pltpu.make_async_copy(x_h.at[tile(t)], g.at[tile(t)], t_sem.at[t])

    def keep_a0(t):
        return pltpu.make_async_copy(a.at[tile(t)], a0_h.at[tile(t)], o_sem.at[t])

    def part_0(which, owner, h=None):
        if which < 2:
            return wgu.at[0, which, of(owner * ROWS, ROWS), pl.ds(0, F) if h is None else of(SUB * h, SUB)]
        return wd.at[0, of(owner * COLS, COLS) if h is None else of(owner * COLS + COLS // 2 * h, COLS // 2)]

    for which, w in enumerate((wg_h, wu_h)):
        for b in range(4):
            cols = pl.ds(b * COLS, COLS)
            pltpu.make_async_copy(w.at[0, :, pl.ds(b * F, COLS)], wgu.at[0, which, of(s * ROWS, ROWS), cols], own0.at[which]).start()
    pltpu.make_async_copy(wd_h.at[0, pl.ds(0, COLS)], part_0(2, s), own0.at[2]).start()

    def route(path):
        theirs = xn["s"]
        return ((s, None, sib), (s, y, xn), (theirs, y, yn), (theirs, y, sib), (theirs, 1 - y, sib))[path]

    def copy_0(path, which):
        owner, h, to = route(path)
        ref = part_0(which, owner, h)
        return remote(ref, ref, gs0.at[path, which], gr0.at[path, which], to)

    for t in range(NT):
        load_x(t).start()
    pl.semaphore_wait(barrier, 6)
    for which in range(3):
        pltpu.make_async_copy(part_0(which, s), part_0(which, s), own0.at[which]).wait()
        copy_0(1, which).start()
        copy_0(0, which).start()

    def part_gu(u, owner, h=None):
        cols = pl.ds(0, F) if h is None else of(SUB * h, SUB)
        return ggu_h.at[u, :, of(owner * ROWS, ROWS), cols]

    def part_d(u, owner, h=None):
        rows = of(owner * COLS, COLS) if h is None else of(owner * COLS + COLS // 2 * h, COLS // 2)
        return gd_h.at[u, rows]

    def own_pieces(u, blocks):
        layer, j = u // J, u % J
        for which, w in enumerate((wg_h, wu_h)):
            for b in blocks:
                yield w.at[layer, :, of(b * F + j * COLS, COLS)], which, of(b * COLS, COLS)

    def own_d(u, h=None):
        layer, j = u // J, u % J
        rows = of(j * COLS, COLS) if h is None else of(j * COLS + COLS // 2 * h, COLS // 2)
        return wd_h.at[layer, rows]

    def send_own(u):
        for h, path, to in ((y, 1, xn), (None, 0, sib)):
            blocks = range(4) if h is None else (2 * h, 2 * h + 1)
            for src, which, cols in own_pieces(u, blocks):
                remote(src, ggu_h.at[u, which, of(s * ROWS, ROWS), cols], gs_sem.at[path, 0], gr_sem.at[u, path, 0], to).start()
            remote(own_d(u, h), part_d(u, s, h), gs_sem.at[path, 1], gr_sem.at[u, path, 1], to).start()

    def gather_copy(u, path, which):
        owner, h, to = route(path)
        ref = (part_gu, part_d)[which](u, owner, h)
        return remote(ref, ref, gs_sem.at[path, which], gr_sem.at[u, path, which], to)

    def gather_sent(path, which):
        owner, h, to = route(path)
        ref = (part_gu, part_d)[which](pl.ds(1, C - 1), owner, h)
        remote(ref, ref, gs_sem.at[path, which], gr_sem.at[0, path, which], to).wait_send()

    def forward_x(u, which):
        gather_copy(u, 1, which).wait_recv()
        gather_copy(u, 2, which).start()
        gather_copy(u, 3, which).start()

    def forward_y(u, which):
        gather_copy(u, 2, which).wait_recv()
        gather_copy(u, 4, which).start()

    def both(fn, u):
        fn(u, 0)
        fn(u, 1)

    def arrived(u, which):
        for path in (0, 3, 4):
            gather_copy(u, path, which).wait_recv()

    def load_gu(u, slot):
        for src, which, cols in own_pieces(u, range(4)):
            pltpu.make_async_copy(src, wgu.at[slot, which, of(s * ROWS, ROWS), cols], w_sem.at[slot, 0]).start()
        for k in (1, 2, 3):
            owner = (s + k) % 4
            pltpu.make_async_copy(part_gu(u, owner), wgu.at[slot, :, of(owner * ROWS, ROWS)], w_sem.at[slot, 0]).start()

    def load_d(u, slot):
        pltpu.make_async_copy(own_d(u), wd.at[slot, of(s * COLS, COLS)], w_sem.at[slot, 1]).start()
        for k in (1, 2, 3):
            owner = (s + k) % 4
            pltpu.make_async_copy(part_d(u, owner), wd.at[slot, of(owner * COLS, COLS)], w_sem.at[slot, 1]).start()

    def loaded(slot, which):
        ref = (wgu, wd)[which].at[slot]
        pltpu.make_async_copy(ref, ref, w_sem.at[slot, which]).wait()

    for u in range(1, 2 * J):
        send_own(u)

    for t in range(NT):
        load_x(t).wait()
        rows = pl.ds(t * T, T)
        a[rows] = normed(g[rows])
        keep_a0(t).start()
        acc[rows] = jnp.zeros((T, D), f32)

    def forward_x0(which):
        copy_0(1, which).wait_recv()
        copy_0(2, which).start()
        copy_0(3, which).start()

    def forward_y0(which):
        copy_0(2, which).wait_recv()
        copy_0(4, which).start()

    with jax.named_scope("w0"):
        for which in range(3):
            forward_x0(which)
        for which in range(2):
            forward_y0(which)
        for which in range(2):
            for path in (0, 3, 4):
                copy_0(path, which).wait_recv()
    save_0 = (
        pltpu.make_async_copy(wgu.at[0], ggu_h.at[0], save_sem.at[0]),
        pltpu.make_async_copy(wd.at[0], gd_h.at[0], save_sem.at[1]),
    )
    save_0[0].start()

    def forward(kept, mid):
        def keep(c, t):
            return pltpu.make_async_copy(kept.at[t % 2], gates_h.at[c, :, tile(t)], gate_sem.at[t % 2])

        def keep_half(c, t, h):
            rows, size = h * (T // 2), T // 2
            to = gates_h.at[c, :, of(t * T + rows, size)]
            return pltpu.make_async_copy(kept.at[t % 2, :, pl.ds(rows, size)], to, gate_sem.at[t % 2])

        def keep_mid(c, t):
            return pltpu.make_async_copy(mid.at[tile(t)], mids_h.at[c, tile(t)], mid_sem.at[t])

        def chunk(c, _):
            slot = c % 2

            @pl.when(c > 0)
            def _():
                with jax.named_scope("wload"):
                    loaded(slot, 0)

            def body(t, _):
                @pl.when(c * NT + t >= 2)
                def _():
                    keep(c, t).wait()

                @pl.when(c > 0)
                def _():
                    keep_mid(c, t).wait()

                with jax.named_scope("ftile"):
                    for i in range(T // SUB):
                        rows, part = of(t * T + i * SUB, SUB), pl.ds(i * SUB, SUB)
                        for cols in HALVES:
                            gate, up = dot(a[rows], wgu[slot, 0, :, cols]), dot(a[rows], wgu[slot, 1, :, cols])
                            sig = 1.0 / (1.0 + jnp.exp(-gate))
                            silu = gate * sig
                            kept[t % 2, 0, part, cols] = silu
                            kept[t % 2, 1, part, cols] = up * (sig + silu * (1.0 - sig))
                            mid[rows, cols] = (silu * up).astype(bf16)
                        if i % 2:
                            keep_half(c, t, i // 2).start()
                keep_mid(c, t).start()

                @pl.when((t == 0) & (c == 0))
                def _():
                    with jax.named_scope("f0"):
                        forward_y0(2)
                        forward_x(1, 0)

                @pl.when((t == 1) & (c == 0))
                def _():
                    with jax.named_scope("f1"):
                        forward_x(1, 1)

                @pl.when((t == 1) & (c > 0))
                def _():
                    with jax.named_scope("fa"):
                        arrived(c, 1)
                        load_d(c, slot)

                @pl.when(t == NT - 1)
                def _():
                    with jax.named_scope("f3"):
                        forward_y(c + 1, 0)

                return 0

            lax.fori_loop(0, NT, body, 0)

            def middle():
                with jax.named_scope("mid"):
                    forward_y(c + 1, 1)
                    arrived(c + 1, 0)

                    @pl.when(c == 1)
                    def _():
                        for copy in save_0:
                            copy.wait()
                        for path in range(5):
                            for which in range(3):
                                copy_0(path, which).wait_send()

                    load_gu(c + 1, 1 - slot)
                    both(forward_x, c + 2)

            @pl.when(c == 0)
            def _():
                for path in (0, 3, 4):
                    copy_0(path, 2).wait_recv()
                save_0[1].start()

            @pl.when(c > 0)
            def _():
                with jax.named_scope("wload"):
                    loaded(slot, 1)

            @pl.when(c < J - 1)
            def _():
                def down(t, _):
                    rows = of(t * 2 * T, 2 * T)
                    acc[rows] += dot(mid[rows], wd[slot])
                    pl.when(t == 0)(middle)
                    return 0

                with jax.named_scope("fdown"):
                    lax.fori_loop(0, N // (2 * T), down, 0)

            @pl.when(c == J - 1)
            def _():
                def down(t, _):
                    keep_a0(t).wait()
                    for i in range(4):
                        rows = of(t * T + i * SUB, SUB)
                        add = (acc[rows] + dot(mid[rows], wd[slot])).astype(bf16)
                        h1 = (g[rows].astype(f32) + add.astype(f32)).astype(bf16)
                        g[rows] = h1
                        a[rows] = normed(h1)
                        acc[rows] = jnp.zeros((SUB, D), f32)
                    put_h1(t).start()
                    pl.when(t == 1)(middle)

                    @pl.when(t == NT - 1)
                    def _():
                        arrived(J, 1)
                        load_d(J, 0)


                    @pl.when(t > 0)
                    def _():
                        put_h1(t - 1).wait()
                        load_dy(t - 1).start()

                    return 0

                with jax.named_scope("fdown1"):
                    lax.fori_loop(0, NT, down, 0)

            return 0

        lax.fori_loop(0, J, chunk, 0)
        for t in range(NT):
            keep_mid(J - 1, t).wait()
        keep(J - 1, 0).wait()
        keep(J - 1, 1).wait()

    def put_h1(t):
        return pltpu.make_async_copy(g.at[tile(t)], h1_h.at[tile(t)], out_sem.at[t])

    def load_dy(t):
        return pltpu.make_async_copy(dy_h.at[tile(t)], g.at[tile(t)], t_sem.at[t])

    def load_h1(t):
        return pltpu.make_async_copy(h1_h.at[tile(t)], a.at[tile(t)], out_sem.at[t])

    def load_a0(t):
        return pltpu.make_async_copy(a0_h.at[tile(t)], a.at[tile(t)], t_sem.at[t])

    pl.run_scoped(forward, pltpu.VMEM((2, 2, T, F), f32), pltpu.VMEM((N, F), bf16))
    put_h1(NT - 1).wait()
    load_dy(NT - 1).start()

    def by_core(p, m):
        return remote(stg.at[p, m, 1 - core], rc.at[p, m], cs.at[p, m], cr.at[p, m], sib)

    def by_x(p, m):
        return remote(xs.at[p, m], rx.at[p, m], xss.at[p, m], xrs.at[p, m], xn)

    def by_y(p, m):
        return remote(ys.at[p, m], ry.at[p, m], yss.at[p, m], yrs.at[p, m], yn)

    def by_z(p, m, k):
        return remote(zs.at[p, m, of((z + k) % 4 * BLOCK, BLOCK)], rz.at[p, m, 3 - k], zss.at[p, m], zrs.at[p, m], zn[k])

    def by_z_all(p, m):
        return remote(zs.at[p, m, pl.ds(0, 3 * BLOCK)], rz.at[p, m], zss.at[p, m], zrs.at[p, m], zn[1])

    def back_z(c, p, m, k):
        ref = fin.at[c, m, of(HALF * y + BLOCK * z, BLOCK)]
        return remote(ref, ref, ass_.at[p, m], ars.at[p, m], zn[k])

    def back_z_all(c, p, m):
        ref = fin.at[c, m, pl.ds(0, 3 * BLOCK)]
        return remote(ref, ref, ass_.at[p, m], ars.at[p, m], zn[1])

    def back_y(c, p, m):
        ref = fin.at[c, m, of(HALF * y, HALF)]
        return remote(ref, ref, bss.at[p, m], brs.at[p, m], yn)

    def s0(c, m, res):
        p = c % 2
        for o in range(4):
            if m == 0:
                stg[p, m, o % 2, o // 2] = res[:, o * COLS : (o + 1) * COLS].astype(bf16)
            else:
                for q in range(4):
                    stg[p, m, o % 2, o // 2, q * ROWS : (q + 1) * ROWS] = res[o * ROWS : (o + 1) * ROWS, q * COLS : (q + 1) * COLS].astype(bf16)
        by_core(p, m).start()

    def s1(c, m):
        p = c % 2
        by_core(p, m).wait()
        xs[p, m] = (stg[p, m, core, 1 - xx].astype(f32) + rc[p, m, 1 - xx].astype(f32)).astype(bf16)
        by_x(p, m).start()

    def s2(c, m):
        p = c % 2
        by_x(p, m).wait()

        def sum_of(h):
            rows = of(HALF * h, HALF)
            return stg[p, m, core, xx, rows].astype(f32) + rc[p, m, xx, rows].astype(f32) + rx[p, m, rows].astype(f32)

        ys[p, m] = sum_of(1 - y).astype(bf16)
        by_y(p, m).start()
        accy[p, m] = sum_of(y)

    def s3(c, m):
        p = c % 2
        by_y(p, m).wait()
        total = accy[p, m] + ry[p, m].astype(f32)
        accy[p, m] = total
        zs[p, m] = total.astype(bf16)
        for k in zn:
            by_z(p, m, k).start()

    def s4(c, m):
        p = c % 2
        by_z_all(p, m).wait_send()
        by_z_all(p, m).wait_recv()
        total = accy[p, m, of(BLOCK * z, BLOCK)]
        for k in range(3):
            total += rz[p, m, k].astype(f32)
        fin[c, m, of(HALF * y + BLOCK * z, BLOCK)] = total.astype(bf16)
        for k in zn:
            back_z(c, p, m, k).start()

    def s5(c, m):
        p = c % 2
        back_z_all(c, p, m).wait()
        back_y(c, p, m).start()

    def put(c, m):
        return pltpu.make_async_copy(fin.at[c, m], grad_h.at[c, m], put_sem.at[0])

    def s6(c, m):
        p = c % 2
        back_y(c, p, m).wait_send()
        other = fin.at[c, m, of(HALF * (1 - y), HALF)]
        remote(other, other, bss.at[p, m], brs.at[p, m], yn).wait_recv()
        put(c, m).start()

    SLOTS = {
        "A0": "121201322",
        "A1": "412502",
        "A2": "422602",
        "A3": "512,100",
        "H0": "211301623",
        "H1": "221,311401,100",
        "H2": "110522612,,311401",
    }
    STEPS = (None, s1, s2, s3, s4, s5, s6)

    def events(name, layer):
        word = (SLOTS[name].split(",") + ["", ""])[layer]
        return [tuple(map(int, word[i : i + 3])) for i in range(0, len(word), 3)]

    def run(name, c):
        with jax.named_scope("slot_" + name):
            for layer, here in enumerate((c >= 0, c >= J, c < J)):
                for back in range(4):
                    todo = [(STEPS[i], m) for i, m, ago in events(name, layer) if ago == back]

                    def do(todo=todo, back=back):
                        for fn, m in todo:
                            fn(c - back, m)

                    if todo and (back or layer):
                        pl.when(here & (c >= back))(do)
                    elif todo:
                        do()

    def ready(i, m, c):
        after = 3.3 * m + (-4.3, 1.4, 5.4, 10.7, 16.0, 20.0)[i - 1]
        return after - 12 * (C - 1 - c)

    def finish():
        left = sorted((ready(i, m, c), i, m, c) for name in SLOTS for i, m, ago in events(name, 0) + events(name, 1) for c in range(C - ago, C))
        sent = [(path, which) for path in range(5) for which in range(2)]
        for n, (_, i, m, c) in enumerate(left):
            with jax.named_scope(f"t{i}_{m}_{c}"):
                STEPS[i](c, m)
            if n < len(sent):
                gather_sent(*sent[n])
        pltpu.make_async_copy(fin, grad_h, put_sem.at[0]).wait()

    def gates(t):
        half = (t % 2) * 2 * T
        return acc.at[of(half, T), pl.ds(0, F)], acc.at[of(half + T, T), pl.ds(0, F)]

    def load_gates(c, t):
        return [
            pltpu.make_async_copy(gates_h.at[c - J, which, tile(t)], to, gate_sem.at[which * 2 + t % 2])
            for which, to in enumerate(gates(t))
        ]

    def backward(act):
        def chunk(c, _):
            slot = c % 2
            with jax.named_scope("wload"):
                loaded(slot, 0)
                loaded(slot, 1)

            def by_gates(rows, cols, gate, up, by_mid):
                by_mid = by_mid.astype(bf16).astype(f32)
                sig = 1.0 / (1.0 + jnp.exp(-gate))
                silu = gate * sig
                act[0, rows, cols] = (silu * up).astype(bf16)
                act[2, rows, cols] = (by_mid * silu).astype(bf16)
                act[1, rows, cols] = (by_mid * up * (sig + silu * (1.0 - sig))).astype(bf16)

            def load_mids(chunk, t):
                return pltpu.make_async_copy(mids_h.at[chunk - J, tile(t)], act.at[0, tile(t)], mid_sem.at[t])

            def product(m):
                lhs, rows, more = (g, a, a)[m], pl.ds(0, N // 2), pl.ds(N // 2, N // 2)
                with jax.named_scope(f"dw{m}"):
                    half[...] = dot(lhs[rows], act[m, rows], TN)
                    s0(c, m, half[...] + dot(lhs[more], act[m, more], TN))
                run(f"H{m}", c)
                if m == 0:

                    @pl.when((c >= J - 1) & (c < C - 1))
                    def _():
                        for t in range(NT):
                            load_mids(c + 1, t).start()

            def body(t, _):
                @pl.when(c < J)
                def _():
                    @pl.when(c == 0)
                    def _():
                        load_dy(t).wait()

                    with jax.named_scope("btile"):
                        for i in range(4):
                            rows = of(t * T + i * SUB, SUB)
                            for cols in HALVES:
                                gate, up = dot(a[rows], wgu[slot, 0, :, cols]), dot(a[rows], wgu[slot, 1, :, cols])
                                by_gates(rows, cols, gate, up, dot(g[rows], wd[slot, cols], TT))

                @pl.when(c >= J)
                def _():
                    with jax.named_scope("gwait"):
                        for copy in load_gates(c, t):
                            copy.wait()
                    with jax.named_scope("ctile"):
                        by_up, by_gate = gates(t)
                        for i in range(T // SUB):
                            rows, part = of(t * T + i * SUB, SUB), pl.ds(i * SUB, SUB)
                            by_mid = dot(g[rows], wd[slot], TT).astype(bf16).astype(f32)
                            act[2, rows] = (by_mid * by_up[part]).astype(bf16)
                            act[1, rows] = (by_mid * by_gate[part]).astype(bf16)

                    @pl.when(t < 2)
                    def _():
                        for copy in load_gates(c, t + 2):
                            copy.start()

                    @pl.when((t >= 2) & (c + 1 < C))
                    def _():
                        for copy in load_gates(c + 1, t - 2):
                            copy.start()

                for k in range(NT):

                    @pl.when(t == k)
                    def _(k=k):
                        run(f"A{k}", c)
                        if k == 1:

                            @pl.when(c >= J)
                            def _():
                                for t in range(NT):
                                    load_mids(c, t).wait()
                                product(0)

                        if k < 3:

                            @pl.when(c == 0)
                            def _():
                                if k == 0:
                                    both(forward_y, J + 1)
                                    both(forward_x, J + 2)
                                if k == 2:
                                    both(forward_x, J + 3)

                            if k == 1:

                                @pl.when(c == 1)
                                def _():
                                    both(forward_y, J + 3)

                        else:

                            @pl.when(c == 0)
                            def _():
                                both(forward_y, J + 2)

                            @pl.when(c + 1 < J)
                            def _():
                                for which in (0, 1):
                                    arrived(J + 1 + c, which)

                            @pl.when(c + 1 < C)
                            def _():
                                u = (c + 1 + J) % C
                                load_gu(u, 1 - slot)
                                load_d(u, 1 - slot)

                return 0

            lax.fori_loop(0, NT, body, 0)

            @pl.when(c == J)
            def _():
                for t in range(NT):
                    load_a0(t).wait()

            pl.when(c < J)(functools.partial(product, 0))
            product(1)
            product(2)

            def by_states(rows):
                return dot(act[1, rows], wgu[slot, 0], TT) + dot(act[2, rows], wgu[slot, 1], TT)

            @pl.when(c < J - 1)
            def _():
                def more(t, _):
                    for i in range(8):
                        rows = of(t * 2 * T + i * SUB, SUB)
                        acc[rows] += by_states(rows)
                    return 0

                with jax.named_scope("p3"):
                    lax.fori_loop(0, N // (2 * T), more, 0)

            @pl.when(c == J - 1)
            def _():
                for t in range(NT):
                    load_h1(t).start()

                def more(t, _):
                    load_h1(t).wait()
                    for i in range(4):
                        rows = of(t * T + i * SUB, SUB)
                        by_a = (acc[rows] + by_states(rows)).astype(bf16).astype(f32)
                        wide = a[rows].astype(f32)
                        scale = lax.rsqrt(jnp.mean(wide * wide, -1, keepdims=True) + 1e-6)
                        along = jnp.mean(by_a * wide, -1, keepdims=True) * (scale * scale * scale)
                        by_h = (by_a * scale - wide * along).astype(bf16)
                        g[rows] = (g[rows].astype(f32) + by_h.astype(f32)).astype(bf16)
                    load_a0(t).start()

                    @pl.when(t % 2 == 1)
                    def _():
                        for copy in load_gates(J, t // 2):
                            copy.start()

                    return 0

                with jax.named_scope("normbwd"):
                    lax.fori_loop(0, NT, more, 0)

            return 0

        lax.fori_loop(0, C, chunk, 0)

    pl.run_scoped(backward, pltpu.VMEM((3, N, F), bf16))
    finish()


def gradients(x, dy, w_gate, w_up, w_down):
    C = L * J
    vmem, dma = pltpu.VMEM, pltpu.SemaphoreType.DMA
    hbm = pl.BlockSpec(memory_space=pl.ANY)
    out = [((C, 2, D, F), bf16), ((C, F, D), bf16), ((N, D), bf16), ((N, D), bf16), ((J, 2, N, F), f32), ((J, N, F), bf16), ((C, 3, D, COLS), bf16)]
    pairs = [dma((2, 3))] * 12
    return pl.pallas_call(
        step_kernel,
        out_shape=[jax.ShapeDtypeStruct(*o) for o in out],
        in_specs=[hbm] * 5,
        out_specs=[hbm] * 7,
        scratch_shapes=[
            vmem((N, D), bf16), vmem((N, D), bf16), vmem((N, D), f32), vmem((D, F), f32),
            vmem((2, 2, D, F), bf16), vmem((2, F, D), bf16),
            vmem((2, 3, 2, 2, D, COLS), bf16), vmem((2, 3, 2, D, COLS), bf16),
            vmem((2, 3, D, COLS), bf16), vmem((2, 3, D, COLS), bf16),
            vmem((2, 3, D // 2, COLS), bf16), vmem((2, 3, D // 2, COLS), bf16), vmem((2, 3, D // 2, COLS), f32),
            vmem((2, 3, D // 2, COLS), bf16), vmem((2, 3, 3, D // 8, COLS), bf16),
            vmem((C, 3, D, COLS), bf16),
            dma((5, 2)), dma((C, 5, 2)), dma((5, 3)), dma((5, 3)), dma((3,)), dma((2,)), dma((2, 2)), dma((NT,)), dma((NT,)), dma((NT,)), dma((4,)), dma((NT,)), dma((1,)),
            *pairs,
        ],
        compiler_params=pltpu.CompilerParams(collective_id=0, has_side_effects=True, vmem_limit_bytes=VLIM * 2**20),
        cost_estimate=pl.CostEstimate(flops=180 * 10**9, bytes_accessed=10**8, transcendentals=4 * 10**7),
        name="step",
    )(x, dy, w_gate, w_up, w_down)[6]


def adamw_kernel(gg, gu, gd, *refs):
    ins, outs = refs[:9], refs[9:]

    def update(which, at, g):
        w, m, v = (ins[k * 3 + which] for k in range(3))
        g = g.astype(f32)
        new_m = 0.9 * m[at] + 0.1 * g
        new_v = 0.95 * v[at] + 0.05 * g * g
        old = w[at].astype(f32)
        step = new_m * lax.rsqrt(new_v + 1e-8) + 0.1 * old
        outs[which][at] = (old - 0.02 * step).astype(bf16)
        outs[3 + which][at] = new_m
        outs[6 + which][at] = new_v

    for which, grad in enumerate((gg, gu)):
        for j in range(J):
            for q in range(4):
                update(which, (0, slice(None), slice(q * F + j * COLS, q * F + (j + 1) * COLS)), grad[0, j, 0, q])
    for j in range(gd.shape[1]):
        update(2, (0, slice(j * COLS, (j + 1) * COLS), slice(None)), gd[0, j, 0].astype(f32).T)


def adamw(grad, weights, m, v):
    parts = 2
    rows = ROWS // parts
    split = grad.reshape(L, J, 3, 4, ROWS, COLS)
    whole = grad.reshape(L, J, 3, D, COLS)
    ff = pl.BlockSpec((1, rows, FF), lambda l, i: (l, i, 0))
    down = pl.BlockSpec((1, FF // 4 // parts, D), lambda l, i: (l, i, 0))
    three = [ff, ff, down]
    shapes = [jax.ShapeDtypeStruct(o.shape, o.dtype) for o in (*weights, *m, *v)]
    return pl.pallas_call(
        adamw_kernel,
        grid=(L, parts),
        out_shape=shapes,
        in_specs=[
            pl.BlockSpec((1, J, 1, 4, rows, COLS), lambda l, i: (1 - l, 0, 1, 0, i, 0)),
            pl.BlockSpec((1, J, 1, 4, rows, COLS), lambda l, i: (1 - l, 0, 2, 0, i, 0)),
            pl.BlockSpec((1, J // parts, 1, D, COLS), lambda l, i: (1 - l, i, 0, 0, 0)),
            *three, *three, *three,
        ],
        out_specs=[*three, *three, *three],
        compiler_params=pltpu.CompilerParams(vmem_limit_bytes=56 * 2**20),
        name="adamw",
    )(split, split, whole, *weights, *m, *v)


def solution(mesh):
    def step(x, dy, *arrays):
        weights, m, v = (arrays[i : i + 3] for i in (0, 3, 6))
        grad = gradients(x[0], dy[0], *weights)
        return tuple(adamw(grad, weights, m, v))

    states, cut = P(("rep", "r", "s"), None, None), P(None, "s", None)
    return jax.shard_map(
        step,
        mesh=mesh,
        in_specs=(states, states) + (cut,) * 9,
        out_specs=(P("rep", "s", None),) * 9,
        check_vma=False,
    )
```
